32 devices in a mesh: dp: 4 (over y, z), dcp: 8 (over x, core).
Axes of the slice: x: 4, y: 2, z: 2, core: 2. Of those that a mesh axis runs over, the one named last changes fastest.
The devices are a block of a 4x4x8 slice.
Arguments:
- q_abs: bfloat16 [1024, 16, 576], P('dp', 'dcp'), parts along dimension 0
- latent_cache: bfloat16 [1024, 1, 8, 128, 576], P('dp', None, 'dcp'), parts along dimension 0
- ctx_len: int32 [1024], P('dp'), parts along dimension 0
Outputs:
- output: bfloat16 [1024, 16, 512], P(('dp', 'dcp')), parts along dimension 0
There are 4 independent parts. The reference program is written for one: setup_inputs(seed, part) draws one part's arguments, and reference() takes and returns one part's arrays. A program takes and returns all parts, laid end to end along the dimension named above; each array names one.
All inputs are finite; a program needn't handle non-finite values.
Results may differ from the reference program's by a relative error of at most 0.00763254.
Values are sent between devices in bfloat16 or wider.
A program may use at most 768 MiB of HBM per device.

```python
import math
import jax
import jax.numpy as jnp
from jax import lax

BATCH_SIZE = 256
NUM_HEADS = 16
LATENT_DIM = 512
ROPE_DIM = 64
NOPE_DIM = 128
PAGES_DEV = 1
GROUP_SIZE = 8
PAGE_LEN = 128

WIDTH = LATENT_DIM + ROPE_DIM
SEQ_LEN = PAGES_DEV * GROUP_SIZE * PAGE_LEN


def setup_inputs(seed: int = 0, part: int = 0) -> dict:
    part_key = jax.random.fold_in(jax.random.key(seed), part)
    key_query, key_cache, key_len = jax.random.split(part_key, 3)
    qk_dim = NOPE_DIM + ROPE_DIM
    cache_rope = 1.4
    query_latent = math.sqrt(0.95 * qk_dim / LATENT_DIM)
    query_rope = math.sqrt(0.95 * qk_dim / ROPE_DIM) / cache_rope
    is_latent = jnp.arange(WIDTH) < LATENT_DIM
    query_scale = jnp.where(is_latent, query_latent, query_rope)
    cache_scale = jnp.where(is_latent, 1.0, cache_rope)
    queries = jax.random.normal(key_query, (BATCH_SIZE, NUM_HEADS, WIDTH), jnp.float32) * query_scale
    cache_vals = jax.random.normal(key_cache, (BATCH_SIZE, PAGES_DEV, GROUP_SIZE, PAGE_LEN, WIDTH), jnp.float32) * cache_scale
    len_drop = jax.random.randint(key_len, (BATCH_SIZE,), 0, SEQ_LEN // 2)
    lengths = jnp.where(jnp.arange(BATCH_SIZE) == 0, SEQ_LEN, SEQ_LEN - len_drop)
    return {'q_abs': queries.astype(jnp.bfloat16), 'latent_cache': cache_vals.astype(jnp.bfloat16), 'ctx_len': lengths.astype(jnp.int32)}


def reference(q_abs, latent_cache, ctx_len):
    inv_scale = (NOPE_DIM + ROPE_DIM) ** -0.5
    q_float = q_abs.astype(jnp.float32)
    per_device = jnp.moveaxis(latent_cache, 2, 0)
    page_base = jnp.arange(PAGES_DEV)[:, None] * (GROUP_SIZE * PAGE_LEN) + jnp.arange(PAGE_LEN)[None, :]

    def one_device(carry_in):
        dev_index, cache_blk = carry_in
        cache_float = cache_blk.astype(jnp.float32)
        scores = jnp.einsum('bhw,bjtw->bhjt', q_float, cache_float) * inv_scale
        positions = page_base + dev_index * PAGE_LEN
        is_valid = positions[None, :, :] < ctx_len[:, None, None]
        scores = jnp.where(is_valid[:, None, :, :], scores, -1e30)
        row_max = jnp.max(scores, axis=(2, 3))
        weights_exp = jnp.exp(scores - row_max[:, :, None, None])
        denom_sum = jnp.sum(weights_exp, axis=(2, 3))
        weights_low = weights_exp.astype(jnp.bfloat16).astype(jnp.float32)
        pv_sum = jnp.einsum('bhjt,bjtc->bhc', weights_low, cache_float[..., :LATENT_DIM])
        part_out = (pv_sum / denom_sum[:, :, None]).astype(jnp.bfloat16)
        part_lse = row_max + jnp.log(denom_sum)
        return part_out, part_lse

    part_outs, part_lses = lax.map(one_device, (jnp.arange(GROUP_SIZE), per_device))
    total_lse = jax.nn.logsumexp(part_lses, axis=0)
    merge_weights = jnp.exp(part_lses - total_lse[None])
    merged = jnp.sum(merge_weights[..., None] * part_outs.astype(jnp.float32), axis=0)
    return merged.astype(jnp.bfloat16)
```

```python
import functools

import jax
import jax.numpy as jnp
from jax import lax
from jax.experimental import pallas as pl
from jax.experimental.pallas import tpu as pltpu
from jax.sharding import PartitionSpec as P

ROPE_DIM = 64
QK_DIM = 192
CORES = 2
STEP = 4
LANES = 128
MESH = pl.DeviceIdType.MESH
F32, BF16 = jnp.float32, jnp.bfloat16


def kernel(group, q_ref, cache_ref, len_ref, out_ref,
           qr, cv, q32, ob, ol, ri, rl, rf, rfl, ff, fl, fb, fbl, fp, fpl,
           q_in, c_in, q_send, q_recv, o_send, r_recv, f_recv, b_recv, p_recv):
    chips = group // CORES
    batch, width, page = cv.shape
    latent = width - ROPE_DIM
    heads = 2 * group
    blk = batch // chips
    core_rows = batch // group
    unit = core_rows // 2
    scale = QK_DIM ** -0.5
    tiles = [(lo, min(lo + LANES, width)) for lo in range(0, width, LANES)]

    me = lax.axis_index('dcp')
    x, k = me // CORES, me % CORES
    xr, xl, xf = (x + 1) % chips, (x + chips - 1) % chips, (x + 2) % chips
    other = 1 - k
    right, left, far, partner = xr * CORES + k, xl * CORES + k, xf * CORES + k, x * CORES + other

    def remote(src, dst, send, recv, dev):
        return pltpu.make_async_remote_copy(src_ref=src, dst_ref=dst, send_sem=send, recv_sem=recv,
                                            device_id={'dcp': dev}, device_id_type=MESH)

    order = [(2, 0, 0), (2, 0, 1), (2, 1, 0), (2, 1, 1),
             (-1, 'o', 0), (1, 'o', 1), (-1, 's', 0), (1, 's', 1),
             (-1, 0, 1), (1, 0, 0), (-1, 1, 1), (1, 1, 0),
             (0, 'o', 0), (0, 'o', 1), (0, 's', 0), (0, 's', 1)]

    def core_of(c):
        return other if c == 'o' else k if c == 's' else c

    def first_row(u):
        r, c, half = order[u]
        return pl.multiple_of((((x + r + chips) % chips) * CORES + core_of(c)) * core_rows + half * unit, unit)

    def cache_copy(u):
        rows = pl.ds(first_row(u), unit)
        return pltpu.make_async_copy(cache_ref.at[rows], cv.at[rows], c_in.at[u])

    own_q = pltpu.make_async_copy(q_ref, qr.at[me], q_in)
    own_q.start()
    for u in range(len(order)):
        cache_copy(u).start()

    barrier = pltpu.get_barrier_semaphore()
    peers = [partner] + [c * CORES + i for c in (xl, xr) for i in range(CORES)]
    for dev in peers:
        pl.semaphore_signal(barrier, inc=1, device_id={'dcp': dev}, device_id_type=MESH)
    pl.semaphore_wait(barrier, len(peers))
    own_q.wait()

    sends = []

    def q_copy(src, y, s, dev, n):
        rows = pl.ds(pl.multiple_of(((y + s) % chips) * blk, blk), blk)
        part = qr.at[src, :, rows, :]
        return remote(part, part, q_send.at[n], q_recv.at[src, s], dev)

    def q_start(src, y, s, dev):
        c = q_copy(src, y, s, dev, len(sends))
        c.start()
        sends.append(c)

    def q_wait(src, y, s):
        q_copy(src, y, s, partner, 0).wait_recv()

    to_right, to_left = [3, 0, 1, 2], [1, 2, 3, 0]
    for i in range(chips):
        q_start(me, x, to_right[i], right)
        q_start(me, x, to_left[i], left)
    for i in range(chips):
        q_start(me, x, i, partner)
    for i in range(chips):
        s = to_right[i]
        q_wait(left, xl, s)
        if s in (0, 1):
            q_start(left, xl, s, right)
        q_start(left, xl, s, partner)
        s = to_left[i]
        q_wait(right, xr, s)
        if s in (2, 3):
            q_start(right, xr, s, left)
        q_start(right, xr, s, partner)
    for s in (0, 2, 1, 3):
        q_wait(far, xf, s)
        q_start(far, xf, s, partner)
    for y in (x, xl, xr, xf):
        for s in range(chips):
            q_wait(y * CORES + other, y, s)

    lane = lax.broadcasted_iota(jnp.int32, (heads, page), 1)
    position = lane + me * page

    def compute(u):
        row0 = first_row(u)
        cache_copy(u).wait()
        for h in range(heads):
            for t, (lo, hi) in enumerate(tiles):
                q32[t, pl.ds(h * unit, unit), pl.ds(0, hi - lo)] = qr[h // 2, h % 2, pl.ds(row0, unit), pl.ds(lo, hi - lo)].astype(F32)

        def body(i, lse):
            for j in range(STEP):
                b = i * STEP + j
                q_b = jnp.concatenate([q32[t, pl.ds(b, heads, stride=unit), :][:, :hi - lo].astype(BF16)
                                       for t, (lo, hi) in enumerate(tiles)], axis=1)
                c_b = cv[row0 + b]
                s = jnp.dot(q_b, c_b, preferred_element_type=F32) * scale
                s = jnp.where(position < len_ref[row0 + b], s, -1e30)
                m = jnp.max(s, axis=1, keepdims=True)
                w = jnp.exp(s - m)
                l = jnp.sum(w, axis=1, keepdims=True)
                o = lax.dot_general(w.astype(BF16), c_b[:latent], (((1,), (1,)), ((), ())),
                                    preferred_element_type=F32)
                ob[u, b] = (o * (1.0 / l)).astype(BF16)
                lse = jnp.where(lane == b, m + jnp.log(l), lse)
            return lse

        ol[u] = lax.fori_loop(0, unit // STEP, body, jnp.zeros((heads, page), F32))

    def combine(terms, store):
        ls = [l[...] for _, l in terms]
        m = functools.reduce(jnp.maximum, ls)
        es = [jnp.exp(l - m) for l in ls]
        total = functools.reduce(jnp.add, es)
        ws = [e * (1.0 / total) for e in es]

        def body(i, carry):
            for j in range(STEP):
                b = i * STEP + j
                acc = None
                for (o, _), w in zip(terms, ws):
                    w_b = jnp.sum(jnp.where(lane == b, w, 0.0), axis=1, keepdims=True)
                    t = w_b * o[b].astype(F32)
                    acc = t if acc is None else acc + t
                store(b, acc)
            return carry

        lax.fori_loop(0, unit // STEP, body, 0)
        return m + jnp.log(total)

    n_out = [0]

    def send(o, l, o_dst, l_dst, sem, dev):
        for src, dst, s in ((o, o_dst, sem.at[0]), (l, l_dst, sem.at[1])):
            c = remote(src, dst, o_send.at[n_out[0]], s, dev)
            c.start()
            n_out[0] += 1
            sends.append(c)

    def arrived(o_dst, l_dst, sem):
        for dst, s in ((o_dst, sem.at[0]), (l_dst, sem.at[1])):
            remote(dst, dst, o_send.at[0], s, partner).wait_recv()

    def relay(way):
        for i in range(3):
            arrived(ri.at[way, i], rl.at[way, i], r_recv.at[way, i])
        mine = order.index((-1, 's', 0) if way == 0 else (1, 's', 1))
        terms = [(ob.at[mine], ol.at[mine])] + [(ri.at[way, i], rl.at[way, i]) for i in range(3)]

        def store(b, acc):
            rf[way, b] = acc

        rfl[way] = combine(terms, store)
        send(rf.at[way], rfl.at[way], ff.at[way], fl.at[way], f_recv.at[way], left if way == 0 else right)

    for u, (r, c, half) in enumerate(order):
        compute(u)
        o, l = ob.at[u], ol.at[u]
        if r == 2:
            dev = (xl if half == 0 else xr) * CORES + c
            send(o, l, ri.at[half, k], rl.at[half, k], r_recv.at[half, k], dev)
        elif r == 0:
            if c == 'o':
                send(o, l, fp.at[half], fpl.at[half], p_recv.at[half], partner)
        elif (r == -1) == (half == 0):
            if c == 'o':
                send(o, l, ri.at[half, 2], rl.at[half, 2], r_recv.at[half, 2], partner)
        else:
            dev = (xl if r == -1 else xr) * CORES + c
            send(o, l, fb.at[half, k], fbl.at[half, k], b_recv.at[half, k], dev)
        if u == 9:
            relay(0)
            relay(1)

    for half in range(2):
        arrived(fp.at[half], fpl.at[half], p_recv.at[half])
        for i in range(CORES):
            arrived(fb.at[half, i], fbl.at[half, i], b_recv.at[half, i])
        arrived(ff.at[half], fl.at[half], f_recv.at[half])
        mine = order.index((0, 's', half))
        terms = [(ob.at[mine], ol.at[mine]), (fp.at[half], fpl.at[half])]
        terms += [(fb.at[half, i], fbl.at[half, i]) for i in range(CORES)]
        terms += [(ff.at[half], fl.at[half])]

        def store(b, acc):
            out_ref[half * unit + b] = acc.astype(BF16)

        combine(terms, store)

    for c in sends:
        c.wait_send()


def solution(mesh):
    group = mesh.shape['dcp']
    chips = group // CORES

    def local_step(q_blk, cache_blk, len_blk):
        batch, _, width = q_blk.shape
        page = cache_blk.shape[3]
        latent = width - ROPE_DIM
        heads = 2 * group
        rows = batch // group
        unit = rows // 2
        units = batch // unit
        q_own = jnp.transpose(q_blk, (1, 0, 2))
        cache_own = jnp.transpose(cache_blk[:, 0, 0], (0, 2, 1))
        any_spec = pl.BlockSpec(memory_space=pl.ANY)
        dma = pltpu.SemaphoreType.DMA
        return pl.pallas_call(
            functools.partial(kernel, group),
            out_shape=jax.ShapeDtypeStruct((rows, heads, latent), BF16),
            in_specs=[any_spec, any_spec, pl.BlockSpec(memory_space=pltpu.SMEM)],
            out_specs=pl.BlockSpec(memory_space=pltpu.VMEM),
            scratch_shapes=[
                pltpu.VMEM((group, 2, batch, width), BF16),
                pltpu.VMEM((batch, width, page), BF16),
                pltpu.VMEM((pl.cdiv(width, LANES), heads * unit, LANES), F32),
                pltpu.VMEM((units, unit, heads, latent), BF16),
                pltpu.VMEM((units, heads, page), F32),
                pltpu.VMEM((2, 3, unit, heads, latent), BF16),
                pltpu.VMEM((2, 3, heads, page), F32),
                pltpu.VMEM((2, unit, heads, latent), F32),
                pltpu.VMEM((2, heads, page), F32),
                pltpu.VMEM((2, unit, heads, latent), F32),
                pltpu.VMEM((2, heads, page), F32),
                pltpu.VMEM((2, CORES, unit, heads, latent), BF16),
                pltpu.VMEM((2, CORES, heads, page), F32),
                pltpu.VMEM((2, unit, heads, latent), BF16),
                pltpu.VMEM((2, heads, page), F32),
                dma(()),
                dma((units,)),
                dma((28,)),
                dma((group, chips)),
                dma((32,)),
                dma((2, 3, 2)),
                dma((2, 2)),
                dma((2, CORES, 2)),
                dma((2, 2)),
            ],
            compiler_params=pltpu.CompilerParams(collective_id=0, has_side_effects=True,
                                                 vmem_limit_bytes=67043328),
        )(q_own, cache_own, len_blk)

    return jax.shard_map(local_step, mesh=mesh, in_specs=(P('dp', 'dcp', None), P('dp', None, 'dcp', None, None), P('dp')), out_specs=P(('dp', 'dcp'), None, None), check_vma=False)
```

```python
import functools

import jax
import jax.numpy as jnp
from jax import lax
from jax.experimental import pallas as pl
from jax.experimental.pallas import tpu as pltpu
from jax.sharding import PartitionSpec as P

ROPE_DIM = 64
QK_DIM = 192
CORES = 2
STEP = 16
MERGE_STEP = 4
LANES = 128
MESH = pl.DeviceIdType.MESH
F32, BF16 = jnp.float32, jnp.bfloat16


def kernel(group, q_ref, cache_ref, len_ref, out_ref,
           qr, cv, q32, sb, wb, ib, ob, ol, ri, rl, rf, rfl, ff, fl, fb, fbl, fp, fpl,
           q_in, c_in, q_send, q_recv, o_send, r_recv, f_recv, b_recv, p_recv):
    chips = group // CORES
    batch, width, page = cv.shape
    latent = width - ROPE_DIM
    heads = 2 * group
    blk = batch // chips
    core_rows = batch // group
    unit = core_rows // 2
    units = batch // unit
    scale = QK_DIM ** -0.5
    tiles = [(lo, min(lo + LANES, width)) for lo in range(0, width, LANES)]

    me = lax.axis_index('dcp')
    x, k = me // CORES, me % CORES
    xr, xl, xf = (x + 1) % chips, (x + chips - 1) % chips, (x + 2) % chips
    other = 1 - k
    right, left, far, partner = xr * CORES + k, xl * CORES + k, xf * CORES + k, x * CORES + other

    def remote(src, dst, send, recv, dev):
        return pltpu.make_async_remote_copy(src_ref=src, dst_ref=dst, send_sem=send, recv_sem=recv,
                                            device_id={'dcp': dev}, device_id_type=MESH)

    order = [(2, 0, 0), (2, 0, 1), (2, 1, 0), (2, 1, 1),
             (-1, 'o', 0), (1, 'o', 1), (-1, 's', 0), (1, 's', 1),
             (-1, 0, 1), (1, 0, 0), (-1, 1, 1), (1, 1, 0),
             (0, 'o', 0), (0, 'o', 1), (0, 's', 0), (0, 's', 1)]

    def core_of(c):
        return other if c == 'o' else k if c == 's' else c

    def first_row(u):
        r, c, half = order[u]
        return pl.multiple_of((((x + r + chips) % chips) * CORES + core_of(c)) * core_rows + half * unit, unit)

    def cache_copy(u):
        rows = pl.ds(first_row(u), unit)
        return pltpu.make_async_copy(cache_ref.at[rows], cv.at[rows], c_in.at[u])

    own_q = pltpu.make_async_copy(q_ref, qr.at[me], q_in)
    own_q.start()
    barrier = pltpu.get_barrier_semaphore()
    peers = [partner] + [c * CORES + i for c in (xl, xr) for i in range(CORES)]
    for dev in peers:
        pl.semaphore_signal(barrier, inc=1, device_id={'dcp': dev}, device_id_type=MESH)
    pl.semaphore_wait(barrier, len(peers))
    own_q.wait()

    sends = []

    def q_copy(src, y, s, dev, n):
        rows = pl.ds(pl.multiple_of(((y + s) % chips) * blk, blk), blk)
        part = qr.at[src, :, rows, :]
        return remote(part, part, q_send.at[n], q_recv.at[src, s], dev)

    def q_start(src, y, s, dev):
        c = q_copy(src, y, s, dev, len(sends))
        c.start()
        sends.append(c)

    def q_wait(src, y, s):
        q_copy(src, y, s, partner, 0).wait_recv()

    to_right, to_left = [3, 0, 1, 2], [1, 2, 3, 0]
    for i in range(chips):
        q_start(me, x, to_right[i], right)
        q_start(me, x, to_left[i], left)
    for i in range(chips):
        q_start(me, x, i, partner)
    for u in range(units):
        cache_copy(u).start()
    for i in range(chips):
        s = to_right[i]
        q_wait(left, xl, s)
        if s in (0, 1):
            q_start(left, xl, s, right)
        q_start(left, xl, s, partner)
        s = to_left[i]
        q_wait(right, xr, s)
        if s in (2, 3):
            q_start(right, xr, s, left)
        q_start(right, xr, s, partner)
    for s in (0, 2, 1, 3):
        q_wait(far, xf, s)
        q_start(far, xf, s, partner)
    for y in (x, xl, xr, xf):
        for s in range(chips):
            q_wait(y * CORES + other, y, s)

    lane = lax.broadcasted_iota(jnp.int32, (heads, page), 1)
    position = lane + me * page

    def stage(t):
        u_qk, u_sm, u_pv = t if t < units else None, t - 1 if 1 <= t <= units else None, t - 2 if t >= 2 else None
        if u_qk is not None:
            row0 = first_row(u_qk)
            cache_copy(u_qk).wait()
            for h in range(heads):
                for c, (lo, hi) in enumerate(tiles):
                    q32[c, pl.ds(h * unit, unit), pl.ds(0, hi - lo)] = qr[h // 2, h % 2, pl.ds(row0, unit), pl.ds(lo, hi - lo)].astype(F32)
        if u_sm is not None:
            sm_row0 = first_row(u_sm)
        if u_pv is not None:
            pv_row0 = first_row(u_pv)

        def body(i, lse):
            for j in range(STEP):
                b = i * STEP + j
                if u_sm is not None:
                    s = sb[u_sm % 2, b] * scale
                    s = jnp.where(position < len_ref[sm_row0 + b], s, -1e30)
                    m = jnp.max(s, axis=1, keepdims=True)
                    w = jnp.exp(s - m)
                    l = jnp.sum(w, axis=1, keepdims=True)
                    lse = jnp.where(lane == b, m + jnp.log(l), lse)
                if u_qk is not None:
                    q_b = jnp.concatenate([q32[c, pl.ds(b, heads, stride=unit), :][:, :hi - lo].astype(BF16)
                                           for c, (lo, hi) in enumerate(tiles)], axis=1)
                    sb[u_qk % 2, b] = jnp.dot(q_b, cv[row0 + b], preferred_element_type=F32)
                if u_pv is not None:
                    o = lax.dot_general(wb[u_pv % 2, b], cv[pv_row0 + b, :latent, :], (((1,), (1,)), ((), ())),
                                        preferred_element_type=F32)
                    ob[u_pv, b] = (o * jnp.concatenate([ib[u_pv % 2, b]] * (latent // page), axis=1)).astype(BF16)
                if u_sm is not None:
                    wb[u_sm % 2, b] = w.astype(BF16)
                    ib[u_sm % 2, b] = jnp.broadcast_to(1.0 / l, (heads, page))
            return lse

        lse = lax.fori_loop(0, unit // STEP, body, jnp.zeros((heads, page), F32))
        if u_sm is not None:
            ol[u_sm] = lse

    def combine(terms, store):
        ls = [l[...] for _, l in terms]
        m = functools.reduce(jnp.maximum, ls)
        es = [jnp.exp(l - m) for l in ls]
        total = functools.reduce(jnp.add, es)
        ws = [e * (1.0 / total) for e in es]

        def body(i, carry):
            for j in range(MERGE_STEP):
                b = i * MERGE_STEP + j
                acc = None
                for (o, _), w in zip(terms, ws):
                    w_b = jnp.sum(jnp.where(lane == b, w, 0.0), axis=1, keepdims=True)
                    t = w_b * o[b].astype(F32)
                    acc = t if acc is None else acc + t
                store(b, acc)
            return carry

        lax.fori_loop(0, unit // MERGE_STEP, body, 0)
        return m + jnp.log(total)

    n_out = [0]

    def send(o, l, o_dst, l_dst, sem, dev):
        for src, dst, s in ((o, o_dst, sem.at[0]), (l, l_dst, sem.at[1])):
            c = remote(src, dst, o_send.at[n_out[0]], s, dev)
            c.start()
            n_out[0] += 1
            sends.append(c)

    def arrived(o_dst, l_dst, sem):
        for dst, s in ((o_dst, sem.at[0]), (l_dst, sem.at[1])):
            remote(dst, dst, o_send.at[0], s, partner).wait_recv()

    def relay(way):
        for i in range(3):
            arrived(ri.at[way, i], rl.at[way, i], r_recv.at[way, i])
        mine = order.index((-1, 's', 0) if way == 0 else (1, 's', 1))
        terms = [(ob.at[mine], ol.at[mine])] + [(ri.at[way, i], rl.at[way, i]) for i in range(3)]

        def store(b, acc):
            rf[way, b] = acc

        rfl[way] = combine(terms, store)
        send(rf.at[way], rfl.at[way], ff.at[way], fl.at[way], f_recv.at[way], left if way == 0 else right)

    for t in range(units + 2):
        stage(t)
        if t < 2:
            continue
        u = t - 2
        r, c, half = order[u]
        o, l = ob.at[u], ol.at[u]
        if r == 2:
            dev = (xl if half == 0 else xr) * CORES + c
            send(o, l, ri.at[half, k], rl.at[half, k], r_recv.at[half, k], dev)
        elif r == 0:
            if c == 'o':
                send(o, l, fp.at[half], fpl.at[half], p_recv.at[half], partner)
        elif (r == -1) == (half == 0):
            if c == 'o':
                send(o, l, ri.at[half, 2], rl.at[half, 2], r_recv.at[half, 2], partner)
        else:
            dev = (xl if r == -1 else xr) * CORES + c
            send(o, l, fb.at[half, k], fbl.at[half, k], b_recv.at[half, k], dev)
        if u == 9:
            relay(0)
            relay(1)

    for half in range(2):
        arrived(fp.at[half], fpl.at[half], p_recv.at[half])
        for i in range(CORES):
            arrived(fb.at[half, i], fbl.at[half, i], b_recv.at[half, i])
        arrived(ff.at[half], fl.at[half], f_recv.at[half])
        mine = order.index((0, 's', half))
        terms = [(ob.at[mine], ol.at[mine]), (fp.at[half], fpl.at[half])]
        terms += [(fb.at[half, i], fbl.at[half, i]) for i in range(CORES)]
        terms += [(ff.at[half], fl.at[half])]

        def store(b, acc):
            out_ref[half * unit + b] = acc.astype(BF16)

        combine(terms, store)

    for c in sends:
        c.wait_send()


def solution(mesh):
    group = mesh.shape['dcp']
    chips = group // CORES

    def local_step(q_blk, cache_blk, len_blk):
        batch, _, width = q_blk.shape
        page = cache_blk.shape[3]
        latent = width - ROPE_DIM
        heads = 2 * group
        rows = batch // group
        unit = rows // 2
        units = batch // unit
        q_own = jnp.transpose(q_blk, (1, 0, 2))
        cache_own = jnp.transpose(cache_blk[:, 0, 0], (0, 2, 1))
        any_spec = pl.BlockSpec(memory_space=pl.ANY)
        dma = pltpu.SemaphoreType.DMA
        return pl.pallas_call(
            functools.partial(kernel, group),
            out_shape=jax.ShapeDtypeStruct((rows, heads, latent), BF16),
            in_specs=[any_spec, any_spec, pl.BlockSpec(memory_space=pltpu.SMEM)],
            out_specs=pl.BlockSpec(memory_space=pltpu.VMEM),
            scratch_shapes=[
                pltpu.VMEM((group, 2, batch, width), BF16),
                pltpu.VMEM((batch, width, page), BF16),
                pltpu.VMEM((pl.cdiv(width, LANES), heads * unit, LANES), F32),
                pltpu.VMEM((2, unit, heads, page), F32),
                pltpu.VMEM((2, unit, heads, page), BF16),
                pltpu.VMEM((2, unit, heads, page), F32),
                pltpu.VMEM((units, unit, heads, latent), BF16),
                pltpu.VMEM((units, heads, page), F32),
                pltpu.VMEM((2, 3, unit, heads, latent), BF16),
                pltpu.VMEM((2, 3, heads, page), F32),
                pltpu.VMEM((2, unit, heads, latent), F32),
                pltpu.VMEM((2, heads, page), F32),
                pltpu.VMEM((2, unit, heads, latent), F32),
                pltpu.VMEM((2, heads, page), F32),
                pltpu.VMEM((2, CORES, unit, heads, latent), BF16),
                pltpu.VMEM((2, CORES, heads, page), F32),
                pltpu.VMEM((2, unit, heads, latent), BF16),
                pltpu.VMEM((2, heads, page), F32),
                dma(()),
                dma((units,)),
                dma((28,)),
                dma((group, chips)),
                dma((32,)),
                dma((2, 3, 2)),
                dma((2, 2)),
                dma((2, CORES, 2)),
                dma((2, 2)),
            ],
            compiler_params=pltpu.CompilerParams(collective_id=0, has_side_effects=True,
                                                 vmem_limit_bytes=67043328),
        )(q_own, cache_own, len_blk)

    return jax.shard_map(local_step, mesh=mesh, in_specs=(P('dp', 'dcp', None), P('dp', None, 'dcp', None, None), P('dp')), out_specs=P(('dp', 'dcp'), None, None), check_vma=False)
```

```python
import functools

import jax
import jax.numpy as jnp
from jax import lax
from jax.experimental import pallas as pl
from jax.experimental.pallas import tpu as pltpu
from jax.sharding import PartitionSpec as P

ROPE_DIM = 64
QK_DIM = 192
CORES = 2
LANES = 128
STEP = 8
MERGE_STEP = 4
PIECES = 2
MESH = pl.DeviceIdType.MESH
F32, BF16 = jnp.float32, jnp.bfloat16

ORDER = [(2, 0, 0), (2, 0, 1), (2, 1, 0), (2, 1, 1),
         (1, 'o', 1), (1, 0, 0), (1, 1, 0), (1, 's', 1),
         (-1, 'o', 0), (-1, 0, 1), (-1, 1, 1), (-1, 's', 0),
         (0, 'o', 0), (0, 'o', 1), (0, 's', 0), (0, 's', 1)]
RELAY_AFTER = 15


def kernel(group, q_ref, cache_ref, len_ref, res,
           qraw, qb0, qb1, qb2, qb3, cv, q32, sb, wb, ib, ob, ol, ri, rl, rf, rfl, ff, fl, fb, fbl, fp, fpl, lo, lol,
           q_in, c_in, q_send, q_recv, o_send, r_recv, f_recv, b_recv, p_recv):
    chips = group // CORES
    batch, width, page = cv.shape
    latent = width - ROPE_DIM
    heads = 2 * group
    blk = batch // chips
    core_rows = batch // group
    unit = core_rows // 2
    units = batch // unit
    piece = unit // PIECES
    scale = QK_DIM ** -0.5

    me = lax.axis_index('dcp')
    x, k = me // CORES, me % CORES
    xr, xl, xf = (x + 1) % chips, (x + chips - 1) % chips, (x + 2) % chips
    other = 1 - k
    right, left, far, partner = xr * CORES + k, xl * CORES + k, xf * CORES + k, x * CORES + other

    def remote(src, dst, send, recv, dev):
        return pltpu.make_async_remote_copy(src_ref=src, dst_ref=dst, send_sem=send, recv_sem=recv,
                                            device_id={'dcp': dev}, device_id_type=MESH)

    def core_of(c):
        return other if c == 'o' else k if c == 's' else c

    def first_row(u):
        r, c, half = ORDER[u]
        return pl.multiple_of((((x + r + chips) % chips) * CORES + core_of(c)) * core_rows + half * unit, unit)

    def cache_copy(u):
        rows = pl.ds(first_row(u), unit)
        return pltpu.make_async_copy(cache_ref.at[rows], cv.at[rows], c_in.at[u])

    blocks = [qb0, qb1, qb2, qb3]
    own_q = pltpu.make_async_copy(q_ref, qraw, q_in)
    own_q.start()

    barrier = pltpu.get_barrier_semaphore()
    peers = [partner] + [c * CORES + i for c in (xl, xr) for i in range(CORES)]
    for dev in peers:
        pl.semaphore_signal(barrier, inc=1, device_id={'dcp': dev}, device_id_type=MESH)

    own_q.wait()
    for s in range(chips):
        first = ((x + s) % chips) * blk
        cols = pl.ds(pl.multiple_of(first // LANES * LANES, LANES), LANES)
        pick = jnp.where(lax.broadcasted_iota(jnp.int32, (blk, LANES), 1) == lax.broadcasted_iota(jnp.int32, (blk, LANES), 0) + first % LANES, 1.0, 0.0).astype(BF16)
        parts = [qraw[h, c * LANES:(c + 1) * LANES, cols] for h in range(2) for c in range(latent // LANES)]
        parts.append(jnp.concatenate([qraw[h, latent:, cols] for h in range(2)], axis=0))
        for c, part in enumerate(parts):
            rows = lax.dot_general(pick, part, (((1,), (1,)), ((), ())), preferred_element_type=F32)
            blocks[s][me, :, c * LANES:(c + 1) * LANES] = rows.astype(BF16)
    pl.semaphore_wait(barrier, len(peers))

    sends = []
    ME, RIGHT, FAR, LEFT = 0, 1, 2, 3

    def q_copy(src, y, s, dev, to, n):
        return remote(blocks[(y + s) % chips].at[src], blocks[(y + s - to) % chips].at[src], q_send.at[n], q_recv.at[src, s], dev)

    def q_start(src, y, s, dev, to):
        c = q_copy(src, y, s, dev, to, len(sends))
        c.start()
        sends.append(c)

    def q_wait(src, y, s):
        q_copy(src, y, s, partner, 0, 0).wait_recv()

    def go(s, to):
        q_start(me, 0, s, {ME: partner, RIGHT: right, LEFT: left}[to], to)

    def take(y, s, then=None):
        src = {RIGHT: right, FAR: far, LEFT: left}[y]
        q_wait(src, y, s)
        if then is not None:
            q_start(src, y, s, {RIGHT: right, LEFT: left}[then], then)
        q_start(src, y, s, partner, 0)

    def from_partner(own, from_left, from_right, from_far):
        for y, c, s in ((ME, x, own), (LEFT, xl, from_left), (RIGHT, xr, from_right), (FAR, xf, from_far)):
            q_wait(c * CORES + other, y, s)

    go(0, RIGHT)
    go(1, LEFT)
    go(3, RIGHT)
    go(3, LEFT)
    go(2, ME)
    go(2, LEFT)
    for u in range(units):
        cache_copy(u).start()
    for s in (1, 3, 0):
        go(s, ME)
    take(LEFT, 0, RIGHT)
    go(1, RIGHT)
    take(RIGHT, 1)
    take(LEFT, 3)
    go(2, RIGHT)
    take(RIGHT, 3, LEFT)
    go(0, LEFT)
    take(FAR, 0)
    take(RIGHT, 2, LEFT)
    from_partner(2, 3, 1, 0)

    def slot4():
        take(LEFT, 1, RIGHT)
        take(FAR, 3)

    def slot5():
        take(LEFT, 2)
        take(RIGHT, 0)
        from_partner(1, 2, 0, 3)

    def slot6():
        take(FAR, 1)
        take(FAR, 2)
        from_partner(3, 0, 2, 1)
        from_partner(0, 1, 3, 2)

    before = {}
    slot4()
    slot5()
    slot6()

    lane = lax.broadcasted_iota(jnp.int32, (heads, page), 1)
    position = lane + me * page
    rope_lane = lax.broadcasted_iota(jnp.int32, (unit, LANES), 1)
    of_head = [rope_lane < ROPE_DIM, rope_lane >= ROPE_DIM]

    def stage(t):
        u_qk, u_sm, u_pv = t if t < units else None, t - 1 if 1 <= t <= units else None, t - 2 if t >= 2 else None
        if u_qk is not None:
            row0 = first_row(u_qk)
            cache_copy(u_qk).wait()
            r, c, half = ORDER[u_qk]
            q_block = blocks[r % chips]
            q_rows = pl.ds(pl.multiple_of(core_of(c) * core_rows + half * unit, unit), unit)

            def fill(d, carry):
                for h in range(2):
                    rows = pl.ds(pl.multiple_of((d * 2 + h) * unit, unit), unit)
                    for c in range(latent // LANES):
                        q32[c, rows, :] = q_block[d, q_rows, pl.ds(h * latent + c * LANES, LANES)].astype(F32)
                    rope = q_block[d, q_rows, pl.ds(2 * latent, LANES)].astype(F32)
                    q32[latent // LANES, rows, :] = jnp.where(of_head[h], rope, 0.0)
                return carry

            lax.fori_loop(0, group, fill, 0)
        if u_sm is not None:
            sm_row0 = first_row(u_sm)
        if u_pv is not None:
            pv_row0 = first_row(u_pv)

        def body(i, lse):
            for j in range(STEP):
                b = i * STEP + j
                if u_sm is not None:
                    s = sb[u_sm % 2, b] * scale
                    s = jnp.where(position < len_ref[sm_row0 + b], s, -1e30)
                    m = jnp.max(s, axis=1, keepdims=True)
                    w = jnp.exp(s - m)
                    l = jnp.sum(w, axis=1, keepdims=True)
                    lse = jnp.where(lane == b, m + jnp.log(l), lse)
                if u_qk is not None:
                    q_b = jnp.concatenate([q32[c, pl.ds(b, heads, stride=unit), :].astype(BF16)
                                           for c in range(latent // LANES + 1)], axis=1)
                    c_b = jnp.concatenate([cv[row0 + b], cv[row0 + b, latent:, :]], axis=0)
                    sb[u_qk % 2, b] = jnp.dot(q_b, c_b, preferred_element_type=F32)
                if u_pv is not None:
                    o = lax.dot_general(wb[u_pv % 2, b], cv[pv_row0 + b, :latent, :], (((1,), (1,)), ((), ())),
                                        preferred_element_type=F32)
                    ob[u_pv, b] = (o * jnp.concatenate([ib[u_pv % 2, b]] * (latent // page), axis=1)).astype(BF16)
                if u_sm is not None:
                    wb[u_sm % 2, b] = w.astype(BF16)
                    ib[u_sm % 2, b] = jnp.broadcast_to(1.0 / l, (heads, page))
            return lse

        lse = lax.fori_loop(0, unit // STEP, body, jnp.zeros((heads, page), F32))
        if u_sm is not None:
            ol[u_sm] = lse

    def weigh(ls):
        m = functools.reduce(jnp.maximum, ls)
        es = [jnp.exp(l - m) for l in ls]
        total = functools.reduce(jnp.add, es)
        return [e * (1.0 / total) for e in es], m + jnp.log(total)

    def merge(outs, ws, first, count, store):
        def body(i, carry):
            for j in range(MERGE_STEP):
                b = first + i * MERGE_STEP + j
                acc = None
                for o, w in zip(outs, ws):
                    w_b = jnp.sum(jnp.where(lane == b, w, 0.0), axis=1, keepdims=True)
                    t = w_b * o[b].astype(F32)
                    acc = t if acc is None else acc + t
                store(b, acc)
            return carry

        lax.fori_loop(0, count // MERGE_STEP, body, 0)

    n_out = [0]

    def send(src, dst, sem, dev):
        c = remote(src, dst, o_send.at[n_out[0]], sem, dev)
        c.start()
        n_out[0] += 1
        sends.append(c)

    def send_pair(o, l, o_dst, l_dst, sem, dev):
        send(o, o_dst, sem.at[0], dev)
        send(l, l_dst, sem.at[1], dev)

    def arrived(dst, sem):
        remote(dst, dst, o_send.at[0], sem, partner).wait_recv()

    def arrived_pair(o_dst, l_dst, sem):
        arrived(o_dst, sem.at[0])
        arrived(l_dst, sem.at[1])

    def relay(way):
        for i in range(3):
            arrived_pair(ri.at[way, i], rl.at[way, i], r_recv.at[way, i])
        mine = ORDER.index((-1, 's', 0) if way == 0 else (1, 's', 1))
        ws, rfl[way] = weigh([ol[mine]] + [rl[way, i] for i in range(3)])
        outs = [ob.at[mine]] + [ri.at[way, i] for i in range(3)]
        dev = left if way == 0 else right

        def store(b, acc):
            rf[way, b] = acc

        for p in range(PIECES):
            rows = pl.ds(p * piece, piece)
            merge(outs, ws, p * piece, piece, store)
            send(rf.at[way, rows], ff.at[way, rows], f_recv.at[way, p], dev)
            if p == 0:
                send(rfl.at[way], fl.at[way], f_recv.at[way, PIECES], dev)

    for t in range(units + 2):
        if t in before:
            before[t]()
        stage(t)
        if t >= 2:
            u = t - 2
            r, c, half = ORDER[u]
            o, l = ob.at[u], ol.at[u]
            if r == 2:
                dev = (xl if half == 0 else xr) * CORES + c
                send_pair(o, l, ri.at[half, k], rl.at[half, k], r_recv.at[half, k], dev)
            elif r == 0:
                if c == 'o':
                    send_pair(o, l, fp.at[half], fpl.at[half], p_recv.at[half], partner)
            elif (r == -1) == (half == 0):
                if c == 'o':
                    send_pair(o, l, ri.at[half, 2], rl.at[half, 2], r_recv.at[half, 2], partner)
            else:
                dev = (xl if r == -1 else xr) * CORES + c
                send_pair(o, l, fb.at[half, k], fbl.at[half, k], b_recv.at[half, k], dev)
        if t == RELAY_AFTER:
            relay(0)
            relay(1)

    for half in range(2):
        arrived_pair(fp.at[half], fpl.at[half], p_recv.at[half])
        for i in range(CORES):
            arrived_pair(fb.at[half, i], fbl.at[half, i], b_recv.at[half, i])
        mine = ORDER.index((0, 's', half))
        ws, lol[half] = weigh([ol[mine], fpl[half]] + [fbl[half, i] for i in range(CORES)])
        outs = [ob.at[mine], fp.at[half]] + [fb.at[half, i] for i in range(CORES)]

        def store_local(b, acc):
            lo[half, b] = acc

        merge(outs, ws, 0, unit, store_local)

    for half in range(2):
        arrived(fl.at[half], f_recv.at[half, PIECES])
    both = [weigh([lol[half], fl[half]])[0] for half in range(2)]
    for p in range(PIECES):
        for half in range(2):
            arrived(ff.at[half, pl.ds(p * piece, piece)], f_recv.at[half, p])

            def store(b, acc):
                res[half * unit + b] = acc.astype(BF16)

            merge([lo.at[half], ff.at[half]], both[half], p * piece, piece, store)

    for c in sends:
        c.wait_send()


def solution(mesh):
    group = mesh.shape['dcp']
    chips = group // CORES

    def local_step(q_blk, cache_blk, len_blk):
        batch, per_core, width = q_blk.shape
        page = cache_blk.shape[3]
        latent = width - ROPE_DIM
        heads = per_core * group
        rows = batch // group
        unit = rows // 2
        units = batch // unit
        q_own = jnp.transpose(q_blk, (1, 2, 0))
        cache_own = jnp.transpose(cache_blk[:, 0, 0], (0, 2, 1))
        any_spec = pl.BlockSpec(memory_space=pl.ANY)
        dma = pltpu.SemaphoreType.DMA
        vmem = pltpu.VMEM
        return pl.pallas_call(
            functools.partial(kernel, group),
            out_shape=jax.ShapeDtypeStruct((rows, heads, latent), BF16),
            in_specs=[any_spec, any_spec, pl.BlockSpec(memory_space=pltpu.SMEM)],
            out_specs=pl.BlockSpec(memory_space=pltpu.VMEM),
            scratch_shapes=[
                vmem((per_core, width, batch), BF16),
                vmem((group, batch // chips, per_core * width), BF16),
                vmem((group, batch // chips, per_core * width), BF16),
                vmem((group, batch // chips, per_core * width), BF16),
                vmem((group, batch // chips, per_core * width), BF16),
                vmem((batch, width, page), BF16),
                vmem((pl.cdiv(width, LANES), heads * unit, LANES), F32),
                vmem((2, unit, heads, page), F32),
                vmem((2, unit, heads, page), BF16),
                vmem((2, unit, heads, page), F32),
                vmem((units, unit, heads, latent), BF16),
                vmem((units, heads, page), F32),
                vmem((2, 3, unit, heads, latent), BF16),
                vmem((2, 3, heads, page), F32),
                vmem((2, unit, heads, latent), F32),
                vmem((2, heads, page), F32),
                vmem((2, unit, heads, latent), F32),
                vmem((2, heads, page), F32),
                vmem((2, CORES, unit, heads, latent), BF16),
                vmem((2, CORES, heads, page), F32),
                vmem((2, unit, heads, latent), BF16),
                vmem((2, heads, page), F32),
                vmem((2, unit, heads, latent), F32),
                vmem((2, heads, page), F32),
                dma(()),
                dma((units,)),
                dma((28,)),
                dma((group, chips)),
                dma((32,)),
                dma((2, 3, 2)),
                dma((2, PIECES + 1)),
                dma((2, CORES, 2)),
                dma((2, 2)),
            ],
            compiler_params=pltpu.CompilerParams(collective_id=0, has_side_effects=True,
                                                 vmem_limit_bytes=67043328),
        )(q_own, cache_own, len_blk)

    return jax.shard_map(local_step, mesh=mesh, in_specs=(P('dp', 'dcp', None), P('dp', None, 'dcp', None, None), P('dp')), out_specs=P(('dp', 'dcp'), None, None), check_vma=False)
```

```python
import functools

import jax
import jax.numpy as jnp
from jax import lax
from jax.experimental import pallas as pl
from jax.experimental.pallas import tpu as pltpu
from jax.sharding import PartitionSpec as P

ROPE_DIM = 64
QK_DIM = 192
CORES = 2
LANES = 128
STEP = 8
MERGE_STEP = 4
PIECES = 2
MESH = pl.DeviceIdType.MESH
F32, BF16 = jnp.float32, jnp.bfloat16

ORDER = [(2, 0, 0), (2, 0, 1), (2, 1, 0), (2, 1, 1),
         (1, 'o', 1), (1, 0, 0), (1, 1, 0), (1, 's', 1),
         (-1, 'o', 0), (-1, 0, 1), (-1, 1, 1), (-1, 's', 0),
         (0, 'o', 0), (0, 'o', 1), (0, 's', 0), (0, 's', 1)]
RELAY_AFTER = 15
HOLD_UNTIL = 5


def kernel(group, q_ref, cache_ref, len_hbm, out_hbm,
           qraw, qb0, qb1, qb2, qb3, cv, q32, sb, wb, ib, ob, ol, ri, rl, rf, rfl, ff, fl, fb, fbl, fp, fpl, lo, lol, len_ref, res,
           l_in, q_in, c_in, q_send, q_recv, o_send, r_recv, f_recv, b_recv, p_recv, o_out):
    chips = group // CORES
    batch, width, page = cv.shape
    latent = width - ROPE_DIM
    heads = 2 * group
    blk = batch // chips
    core_rows = batch // group
    unit = core_rows // 2
    units = batch // unit
    piece = unit // PIECES
    scale = QK_DIM ** -0.5

    me = lax.axis_index('dcp')
    x, k = me // CORES, me % CORES
    xr, xl = (x + 1) % chips, (x + chips - 1) % chips
    other = 1 - k
    right, left, partner = xr * CORES + k, xl * CORES + k, x * CORES + other

    def remote(src, dst, send, recv, dev):
        return pltpu.make_async_remote_copy(src_ref=src, dst_ref=dst, send_sem=send, recv_sem=recv,
                                            device_id={'dcp': dev}, device_id_type=MESH)

    def core_of(c):
        return other if c == 'o' else k if c == 's' else c

    def first_row(u):
        r, c, half = ORDER[u]
        return pl.multiple_of((((x + r + chips) % chips) * CORES + core_of(c)) * core_rows + half * unit, unit)

    def cache_copy(u):
        rows = pl.ds(first_row(u), unit)
        return pltpu.make_async_copy(cache_ref.at[rows], cv.at[rows], c_in.at[u])

    blocks = [qb0, qb1, qb2, qb3]
    own_q = pltpu.make_async_copy(q_ref, qraw, q_in)
    own_q.start()
    own_len = pltpu.make_async_copy(len_hbm, len_ref, l_in)
    own_len.start()

    barrier = pltpu.get_barrier_semaphore()
    peers = [partner] + [c * CORES + i for c in (xl, xr) for i in range(CORES)]
    for dev in peers:
        pl.semaphore_signal(barrier, inc=1, device_id={'dcp': dev}, device_id_type=MESH)

    own_q.wait()
    for s in range(chips):
        first = ((x + s) % chips) * blk
        cols = pl.ds(pl.multiple_of(first // LANES * LANES, LANES), LANES)
        pick = jnp.where(lax.broadcasted_iota(jnp.int32, (blk, LANES), 1) == lax.broadcasted_iota(jnp.int32, (blk, LANES), 0) + first % LANES, 1.0, 0.0).astype(BF16)
        parts = [qraw[h, c * LANES:(c + 1) * LANES, cols] for h in range(2) for c in range(latent // LANES)]
        parts.append(jnp.concatenate([qraw[h, latent:, cols] for h in range(2)], axis=0))
        for c, part in enumerate(parts):
            rows = lax.dot_general(pick, part, (((1,), (1,)), ((), ())), preferred_element_type=F32)
            blocks[s][0, :, c * LANES:(c + 1) * LANES] = rows.astype(BF16)
    pl.semaphore_wait(barrier, len(peers))

    sends = []
    ME, RIGHT, FAR, LEFT = 0, 1, 2, 3

    def q_copy(y, col, s, dev, to, to_col, n):
        dst = (y - to) % chips * CORES + to_col
        return remote(blocks[(y + s) % chips].at[y * CORES + col], blocks[(y + s - to) % chips].at[dst],
                      q_send.at[n], q_recv.at[dst, s], dev)

    def q_start(y, s, to):
        dev = {ME: partner, RIGHT: right, LEFT: left}[to]
        c = q_copy(y, 0, s, dev, to, 1 if to == ME else 0, len(sends))
        c.start()
        sends.append(c)

    def q_wait(y, col, s):
        q_copy(y, col, s, partner, 0, col, 0).wait_recv()

    def go(s, to):
        q_start(ME, s, to)

    def take(y, s, then=None):
        q_wait(y, 0, s)
        if then is not None:
            q_start(y, s, then)
        q_start(y, s, ME)

    def from_partner(own, from_left, from_right, from_far):
        for y, s in ((ME, own), (LEFT, from_left), (RIGHT, from_right), (FAR, from_far)):
            q_wait(y, 1, s)

    go(0, RIGHT)
    go(1, LEFT)
    go(3, RIGHT)
    go(3, LEFT)
    go(2, ME)
    go(2, LEFT)
    for u in range(units):
        cache_copy(u).start()
    for s in (1, 3, 0):
        go(s, ME)
    take(LEFT, 0, RIGHT)
    go(1, RIGHT)
    take(RIGHT, 1)
    take(LEFT, 3)
    go(2, RIGHT)
    take(RIGHT, 3, LEFT)
    go(0, LEFT)
    take(FAR, 0)
    take(RIGHT, 2, LEFT)
    from_partner(2, 3, 1, 0)

    own_len.wait()
    held = []

    def slot4():
        take(LEFT, 1, RIGHT)
        take(FAR, 3)

    def slot5():
        take(LEFT, 2)
        take(RIGHT, 0)

    def next_block():
        from_partner(1, 2, 0, 3)

    def slot6():
        take(FAR, 1)
        take(FAR, 2)
        for start in held:
            start()

    def last_blocks():
        from_partner(3, 0, 2, 1)
        from_partner(0, 1, 3, 2)

    before = {2: [slot4], 3: [slot5], 4: [next_block], HOLD_UNTIL: [slot6], 8: [last_blocks]}

    lane = lax.broadcasted_iota(jnp.int32, (heads, page), 1)
    position = lane + me * page
    rope_lane = lax.broadcasted_iota(jnp.int32, (unit, LANES), 1)
    of_head = [rope_lane < ROPE_DIM, rope_lane >= ROPE_DIM]

    def stage(t):
        u_qk, u_sm, u_pv = t if t < units else None, t - 1 if 1 <= t <= units else None, t - 2 if t >= 2 else None
        if u_qk is not None:
            row0 = first_row(u_qk)
            cache_copy(u_qk).wait()
            r, c, half = ORDER[u_qk]
            q_block = blocks[r % chips]
            q_rows = pl.ds(pl.multiple_of(core_of(c) * core_rows + half * unit, unit), unit)

            def fill(e, carry):
                d = (x + e // CORES) % chips * CORES + (k + e) % CORES
                for h in range(2):
                    rows = pl.ds(pl.multiple_of((d * 2 + h) * unit, unit), unit)
                    for c in range(latent // LANES):
                        q32[c, rows, :] = q_block[e, q_rows, pl.ds(h * latent + c * LANES, LANES)].astype(F32)
                    rope = q_block[e, q_rows, pl.ds(2 * latent, LANES)].astype(F32)
                    q32[latent // LANES, rows, :] = jnp.where(of_head[h], rope, 0.0)
                return carry

            lax.fori_loop(0, group, fill, 0)
        if u_sm is not None:
            sm_row0 = first_row(u_sm)
        if u_pv is not None:
            pv_row0 = first_row(u_pv)

        def body(i, lse):
            for j in range(STEP):
                b = i * STEP + j
                if u_sm is not None:
                    s = sb[u_sm % 2, b] * scale
                    s = jnp.where(position < len_ref[sm_row0 + b], s, -1e30)
                    m = jnp.max(s, axis=1, keepdims=True)
                    w = jnp.exp(s - m)
                    l = jnp.sum(w, axis=1, keepdims=True)
                    lse = jnp.where(lane == b, m + jnp.log(l), lse)
                if u_qk is not None:
                    q_b = jnp.concatenate([q32[c, pl.ds(b, heads, stride=unit), :].astype(BF16)
                                           for c in range(latent // LANES + 1)], axis=1)
                    c_b = jnp.concatenate([cv[row0 + b], cv[row0 + b, latent:, :]], axis=0)
                    sb[u_qk % 2, b] = jnp.dot(q_b, c_b, preferred_element_type=F32)
                if u_pv is not None:
                    o = lax.dot_general(wb[u_pv % 2, b], cv[pv_row0 + b, :latent, :], (((1,), (1,)), ((), ())),
                                        preferred_element_type=F32)
                    ob[u_pv, b] = (o * jnp.concatenate([ib[u_pv % 2, b]] * (latent // page), axis=1)).astype(BF16)
                if u_sm is not None:
                    wb[u_sm % 2, b] = w.astype(BF16)
                    ib[u_sm % 2, b] = jnp.broadcast_to(1.0 / l, (heads, page))
            return lse

        lse = lax.fori_loop(0, unit // STEP, body, jnp.zeros((heads, page), F32))
        if u_sm is not None:
            ol[u_sm] = lse

    def weigh(ls):
        m = functools.reduce(jnp.maximum, ls)
        es = [jnp.exp(l - m) for l in ls]
        total = functools.reduce(jnp.add, es)
        return [e * (1.0 / total) for e in es], m + jnp.log(total)

    def merge(outs, ws, first, count, store):
        def body(i, carry):
            for j in range(MERGE_STEP):
                b = first + i * MERGE_STEP + j
                acc = None
                for o, w in zip(outs, ws):
                    w_b = jnp.sum(jnp.where(lane == b, w, 0.0), axis=1, keepdims=True)
                    t = w_b * o[b].astype(F32)
                    acc = t if acc is None else acc + t
                store(b, acc)
            return carry

        lax.fori_loop(0, count // MERGE_STEP, body, 0)

    n_out = [0]

    def send(src, dst, sem, dev):
        c = remote(src, dst, o_send.at[n_out[0]], sem, dev)
        c.start()
        n_out[0] += 1
        sends.append(c)

    def send_pair(o, l, o_dst, l_dst, sem, dev):
        send(o, o_dst, sem.at[0], dev)
        send(l, l_dst, sem.at[1], dev)

    def arrived(dst, sem):
        remote(dst, dst, o_send.at[0], sem, partner).wait_recv()

    def arrived_pair(o_dst, l_dst, sem):
        arrived(o_dst, sem.at[0])
        arrived(l_dst, sem.at[1])

    def send_unit(u):
        r, c, half = ORDER[u]
        o, l = ob.at[u], ol.at[u]
        if r == 2:
            dev = (xl if half == 0 else xr) * CORES + c
            send_pair(o, l, ri.at[half, k], rl.at[half, k], r_recv.at[half, k], dev)
        elif r == 0:
            if c == 'o':
                send_pair(o, l, fp.at[half], fpl.at[half], p_recv.at[half], partner)
        elif (r == -1) == (half == 0):
            if c == 'o':
                send_pair(o, l, ri.at[half, 2], rl.at[half, 2], r_recv.at[half, 2], partner)
        else:
            dev = (xl if r == -1 else xr) * CORES + c
            send_pair(o, l, fb.at[half, k], fbl.at[half, k], b_recv.at[half, k], dev)

    def relay(way):
        for i in range(3):
            arrived_pair(ri.at[way, i], rl.at[way, i], r_recv.at[way, i])
        mine = ORDER.index((-1, 's', 0) if way == 0 else (1, 's', 1))
        ws, rfl[way] = weigh([ol[mine]] + [rl[way, i] for i in range(3)])
        outs = [ob.at[mine]] + [ri.at[way, i] for i in range(3)]
        dev = left if way == 0 else right

        def store(b, acc):
            rf[way, b] = acc

        for p in range(PIECES):
            rows = pl.ds(p * piece, piece)
            merge(outs, ws, p * piece, piece, store)
            send(rf.at[way, rows], ff.at[way, rows], f_recv.at[way, p], dev)
            if p == 0:
                send(rfl.at[way], fl.at[way], f_recv.at[way, PIECES], dev)

    for t in range(units + 2):
        for event in before.get(t, []):
            event()
        stage(t)
        if t >= 2:
            u = t - 2
            start = functools.partial(send_unit, u)
            if t < HOLD_UNTIL:
                held.append(start)
            else:
                start()
        if t == RELAY_AFTER:
            relay(0)
            relay(1)

    for half in range(2):
        arrived_pair(fp.at[half], fpl.at[half], p_recv.at[half])
        for i in range(CORES):
            arrived_pair(fb.at[half, i], fbl.at[half, i], b_recv.at[half, i])
        mine = ORDER.index((0, 's', half))
        ws, lol[half] = weigh([ol[mine], fpl[half]] + [fbl[half, i] for i in range(CORES)])
        outs = [ob.at[mine], fp.at[half]] + [fb.at[half, i] for i in range(CORES)]

        def store_local(b, acc):
            lo[half, b] = acc

        merge(outs, ws, 0, unit, store_local)

    for half in range(2):
        arrived(fl.at[half], f_recv.at[half, PIECES])
    done = []
    both = [weigh([lol[half], fl[half]])[0] for half in range(2)]
    for p in range(PIECES):
        for half in range(2):
            arrived(ff.at[half, pl.ds(p * piece, piece)], f_recv.at[half, p])

            def store(b, acc):
                res[half * unit + b] = acc.astype(BF16)

            merge([lo.at[half], ff.at[half]], both[half], p * piece, piece, store)
            rows = pl.ds(half * unit + p * piece, piece)
            c = pltpu.make_async_copy(res.at[rows], out_hbm.at[rows], o_out.at[half, p])
            c.start()
            done.append(c)

    for c in sends:
        c.wait_send()
    for c in done:
        c.wait()


def solution(mesh):
    group = mesh.shape['dcp']
    chips = group // CORES

    def local_step(q_blk, cache_blk, len_blk):
        batch, per_core, width = q_blk.shape
        page = cache_blk.shape[3]
        latent = width - ROPE_DIM
        heads = per_core * group
        rows = batch // group
        unit = rows // 2
        units = batch // unit
        q_own = jnp.transpose(q_blk, (1, 2, 0))
        cache_own = jnp.transpose(cache_blk[:, 0, 0], (0, 2, 1))
        any_spec = pl.BlockSpec(memory_space=pl.ANY)
        dma = pltpu.SemaphoreType.DMA
        vmem = pltpu.VMEM
        return pl.pallas_call(
            functools.partial(kernel, group),
            out_shape=jax.ShapeDtypeStruct((rows, heads, latent), BF16),
            in_specs=[any_spec] * 3,
            out_specs=any_spec,
            scratch_shapes=[
                vmem((per_core, width, batch), BF16),
                vmem((group, batch // chips, per_core * width), BF16),
                vmem((group, batch // chips, per_core * width), BF16),
                vmem((group, batch // chips, per_core * width), BF16),
                vmem((group, batch // chips, per_core * width), BF16),
                vmem((batch, width, page), BF16),
                vmem((pl.cdiv(width, LANES), heads * unit, LANES), F32),
                vmem((2, unit, heads, page), F32),
                vmem((2, unit, heads, page), BF16),
                vmem((2, unit, heads, page), F32),
                vmem((units, unit, heads, latent), BF16),
                vmem((units, heads, page), F32),
                vmem((2, 3, unit, heads, latent), BF16),
                vmem((2, 3, heads, page), F32),
                vmem((2, unit, heads, latent), F32),
                vmem((2, heads, page), F32),
                vmem((2, unit, heads, latent), F32),
                vmem((2, heads, page), F32),
                vmem((2, CORES, unit, heads, latent), BF16),
                vmem((2, CORES, heads, page), F32),
                vmem((2, unit, heads, latent), BF16),
                vmem((2, heads, page), F32),
                vmem((2, unit, heads, latent), F32),
                vmem((2, heads, page), F32),
                pltpu.SMEM((batch,), jnp.int32),
                vmem((rows, heads, latent), BF16),
                dma(()),
                dma(()),
                dma((units,)),
                dma((28,)),
                dma((group, chips)),
                dma((32,)),
                dma((2, 3, 2)),
                dma((2, PIECES + 1)),
                dma((2, CORES, 2)),
                dma((2, 2)),
                dma((2, PIECES)),
            ],
            compiler_params=pltpu.CompilerParams(collective_id=0, has_side_effects=True,
                                                 vmem_limit_bytes=67043328),
        )(q_own, cache_own, len_blk)

    return jax.shard_map(local_step, mesh=mesh, in_specs=(P('dp', 'dcp', None), P('dp', None, 'dcp', None, None), P('dp')), out_specs=P(('dp', 'dcp'), None, None), check_vma=False)
```

```python
import functools

import jax
import jax.numpy as jnp
from jax import lax
from jax.experimental import pallas as pl
from jax.experimental.pallas import tpu as pltpu
from jax.sharding import PartitionSpec as P

ROPE_DIM = 64
QK_DIM = 192
CORES = 2
LANES = 128
STEP = 8
MERGE_STEP = 4
PIECES = 2
MESH = pl.DeviceIdType.MESH
F32, BF16 = jnp.float32, jnp.bfloat16

ORDER = [(2, 0, 0), (2, 0, 1), (2, 1, 0), (2, 1, 1),
         (1, 'o', 1), (1, 0, 0), (1, 1, 0), (1, 's', 1),
         (-1, 'o', 0), (-1, 0, 1), (-1, 1, 1), (-1, 's', 0),
         (0, 'o', 0), (0, 'o', 1), (0, 's', 0), (0, 's', 1)]
RELAY_AFTER = 15
HOLD_UNTIL = 4
TAIL = 16


def kernel(group, q_ref, cache_ref, len_hbm, out_hbm,
           qraw, qb0, qb1, qb2, qb3, cv, q32, sb, wb, ib, ob, ol, ri, rl, rf, rfl, ff, fl, fb, fbl, fp, fpl, lo, lol, len_ref, res,
           l_in, q_in, c_in, q_send, q_recv, q_tail, o_send, r_recv, f_recv, b_recv, p_recv, o_out):
    chips = group // CORES
    batch, width, page = cv.shape
    latent = width - ROPE_DIM
    heads = 2 * group
    blk = batch // chips
    core_rows = batch // group
    unit = core_rows // 2
    units = batch // unit
    piece = unit // PIECES
    scale = QK_DIM ** -0.5

    me = lax.axis_index('dcp')
    x, k = me // CORES, me % CORES
    xr, xl = (x + 1) % chips, (x + chips - 1) % chips
    other = 1 - k
    right, left, partner = xr * CORES + k, xl * CORES + k, x * CORES + other

    def remote(src, dst, send, recv, dev):
        return pltpu.make_async_remote_copy(src_ref=src, dst_ref=dst, send_sem=send, recv_sem=recv,
                                            device_id={'dcp': dev}, device_id_type=MESH)

    def core_of(c):
        return other if c == 'o' else k if c == 's' else c

    def first_row(u):
        r, c, half = ORDER[u]
        return pl.multiple_of((((x + r + chips) % chips) * CORES + core_of(c)) * core_rows + half * unit, unit)

    def cache_copy(u):
        rows = pl.ds(first_row(u), unit)
        return pltpu.make_async_copy(cache_ref.at[rows], cv.at[rows], c_in.at[u])

    blocks = [qb0, qb1, qb2, qb3]
    own_q = pltpu.make_async_copy(q_ref, qraw, q_in)
    own_q.start()
    own_len = pltpu.make_async_copy(len_hbm, len_ref, l_in)
    own_len.start()

    barrier = pltpu.get_barrier_semaphore()
    peers = [partner] + [c * CORES + i for c in (xl, xr) for i in range(CORES)]
    for dev in peers:
        pl.semaphore_signal(barrier, inc=1, device_id={'dcp': dev}, device_id_type=MESH)

    own_q.wait()
    for s in range(chips):
        first = ((x + s) % chips) * blk
        cols = pl.ds(pl.multiple_of(first // LANES * LANES, LANES), LANES)
        pick = jnp.where(lax.broadcasted_iota(jnp.int32, (blk, LANES), 1) == lax.broadcasted_iota(jnp.int32, (blk, LANES), 0) + first % LANES, 1.0, 0.0).astype(BF16)
        parts = [qraw[h, c * LANES:(c + 1) * LANES, cols] for h in range(2) for c in range(latent // LANES)]
        parts.append(jnp.concatenate([qraw[h, latent:, cols] for h in range(2)], axis=0))
        for c, part in enumerate(parts):
            rows = lax.dot_general(pick, part, (((1,), (1,)), ((), ())), preferred_element_type=F32)
            blocks[s][0, :, c * LANES:(c + 1) * LANES] = rows.astype(BF16)
    pl.semaphore_wait(barrier, len(peers))

    sends = []
    ME, RIGHT, FAR, LEFT = 0, 1, 2, 3

    lead = blk - TAIL

    def q_copy(y, col, s, dev, to, to_col, n, sem=None, rows=slice(None)):
        dst = (y - to) % chips * CORES + to_col
        if isinstance(rows, slice):
            rows = pl.ds(0, lead if y - to in (FAR, -FAR) and s in (1, 2) else blk)
        return remote(blocks[(y + s) % chips].at[y * CORES + col, rows], blocks[(y + s - to) % chips].at[dst, rows],
                      q_send.at[n], q_recv.at[dst, s] if sem is None else sem, dev)

    def q_begin(c):
        c.start()
        sends.append(c)

    def q_start(y, s, to):
        dev = {ME: partner, RIGHT: right, LEFT: left}[to]
        q_begin(q_copy(y, 0, s, dev, to, 1 if to == ME else 0, len(sends)))

    def q_wait(y, col, s):
        q_copy(y, col, s, partner, 0, col, 0).wait_recv()

    def go(s, to):
        q_start(ME, s, to)

    def take(y, s, then=None, tail=None):
        q_wait(y, 0, s)
        if then is not None:
            q_start(y, s, then)
        if tail is not None:
            chip = {RIGHT: xr, LEFT: xl}[then]
            for col, core in ((0, k), (1, other)):
                q_begin(q_copy(y, 0, s, chip * CORES + core, then, col, len(sends), q_tail.at[col, tail], pl.ds(lead, TAIL)))
        q_start(y, s, ME)

    def tails():
        for tail, s in ((0, 1), (1, 2)):
            for col in range(CORES):
                q_copy(FAR, col, s, partner, 0, col, 0, q_tail.at[col, tail], pl.ds(lead, TAIL)).wait_recv()

    def from_partner(own, from_left, from_right, from_far):
        for y, s in ((ME, own), (LEFT, from_left), (RIGHT, from_right), (FAR, from_far)):
            q_wait(y, 1, s)

    go(0, RIGHT)
    go(1, LEFT)
    go(3, RIGHT)
    go(3, LEFT)
    go(2, ME)
    go(2, LEFT)
    for u in range(units):
        cache_copy(u).start()
    for s in (1, 3, 0):
        go(s, ME)
    take(LEFT, 0, RIGHT)
    go(1, RIGHT)
    take(RIGHT, 1)
    take(LEFT, 3)
    go(2, RIGHT)
    take(RIGHT, 3, LEFT)
    go(0, LEFT)
    take(FAR, 0)
    take(RIGHT, 2, LEFT, 1)
    from_partner(2, 3, 1, 0)

    own_len.wait()
    held = []

    def slot4():
        take(LEFT, 1, RIGHT, 0)
        take(FAR, 3)

    def slot5():
        take(LEFT, 2)
        take(RIGHT, 0)

    def next_block():
        from_partner(1, 2, 0, 3)

    def slot6():
        take(FAR, 1)
        take(FAR, 2)
        for start in held:
            start()

    def last_blocks():
        tails()
        from_partner(3, 0, 2, 1)
        from_partner(0, 1, 3, 2)

    before = {2: [slot4], 3: [slot5], 4: [slot6, next_block], 8: [last_blocks]}

    lane = lax.broadcasted_iota(jnp.int32, (heads, page), 1)
    position = lane + me * page
    lse_rows = heads // 2
    lse_lane = lax.broadcasted_iota(jnp.int32, (lse_rows, LANES), 1)
    rope_lane = lax.broadcasted_iota(jnp.int32, (unit, LANES), 1)
    of_head = [rope_lane < ROPE_DIM, rope_lane >= ROPE_DIM]

    def stage(t):
        u_qk, u_sm, u_pv = t if t < units else None, t - 1 if 1 <= t <= units else None, t - 2 if t >= 2 else None
        if u_qk is not None:
            row0 = first_row(u_qk)
            cache_copy(u_qk).wait()
            r, c, half = ORDER[u_qk]
            q_block = blocks[r % chips]
            q_rows = pl.ds(pl.multiple_of(core_of(c) * core_rows + half * unit, unit), unit)

            def fill(e, carry):
                d = (x + e // CORES) % chips * CORES + (k + e) % CORES
                for h in range(2):
                    rows = pl.ds(pl.multiple_of((d * 2 + h) * unit, unit), unit)
                    for c in range(latent // LANES):
                        q32[c, rows, :] = q_block[e, q_rows, pl.ds(h * latent + c * LANES, LANES)].astype(F32)
                    rope = q_block[e, q_rows, pl.ds(2 * latent, LANES)].astype(F32)
                    q32[latent // LANES, rows, :] = jnp.where(of_head[h], rope, 0.0)
                return carry

            lax.fori_loop(0, group, fill, 0)
        if u_sm is not None:
            sm_row0 = first_row(u_sm)
        if u_pv is not None:
            pv_row0 = first_row(u_pv)

        def body(i, lse):
            for j in range(STEP):
                b = i * STEP + j
                if u_sm is not None:
                    s = sb[u_sm % 2, b] * scale
                    s = jnp.where(position < len_ref[sm_row0 + b], s, -1e30)
                    m = jnp.max(s, axis=1, keepdims=True)
                    w = jnp.exp(s - m)
                    l = jnp.sum(w, axis=1, keepdims=True)
                    lse_b = m + jnp.log(l)
                    lse = jnp.where(lse_lane == b, lse_b[:lse_rows], jnp.where(lse_lane == b + unit, lse_b[lse_rows:], lse))
                if u_qk is not None:
                    q_b = jnp.concatenate([q32[c, pl.ds(b, heads, stride=unit), :].astype(BF16)
                                           for c in range(latent // LANES + 1)], axis=1)
                    c_b = jnp.concatenate([cv[row0 + b], cv[row0 + b, latent:, :]], axis=0)
                    sb[u_qk % 2, b] = jnp.dot(q_b, c_b, preferred_element_type=F32)
                if u_pv is not None:
                    o = lax.dot_general(wb[u_pv % 2, b], cv[pv_row0 + b, :latent, :], (((1,), (1,)), ((), ())),
                                        preferred_element_type=F32)
                    ob[u_pv, b] = (o * jnp.concatenate([ib[u_pv % 2, b]] * (latent // page), axis=1)).astype(BF16)
                if u_sm is not None:
                    wb[u_sm % 2, b] = w.astype(BF16)
                    ib[u_sm % 2, b] = jnp.broadcast_to(1.0 / l, (heads, page))
            return lse

        lse = lax.fori_loop(0, unit // STEP, body, jnp.zeros((lse_rows, LANES), F32))
        if u_sm is not None:
            ol[u_sm] = lse

    def weigh(ls):
        m = functools.reduce(jnp.maximum, ls)
        es = [jnp.exp(l - m) for l in ls]
        total = functools.reduce(jnp.add, es)
        return [e * (1.0 / total) for e in es], m + jnp.log(total)

    def merge(outs, ws, first, count, store):
        def body(n, carry):
            for j in range(MERGE_STEP):
                b = first + n * MERGE_STEP + j
                acc = None
                for o, w in zip(outs, ws):
                    w_b = jnp.concatenate([jnp.sum(jnp.where(lse_lane == b + i * unit, w, 0.0), axis=1, keepdims=True)
                                           for i in range(2)], axis=0)
                    t = w_b * o[b].astype(F32)
                    acc = t if acc is None else acc + t
                store(b, acc)
            return carry

        lax.fori_loop(0, count // MERGE_STEP, body, 0)

    n_out = [0]

    def send(src, dst, sem, dev):
        c = remote(src, dst, o_send.at[n_out[0]], sem, dev)
        c.start()
        n_out[0] += 1
        sends.append(c)

    def send_pair(o, l, o_dst, l_dst, sem, dev):
        send(o, o_dst, sem.at[0], dev)
        send(l, l_dst, sem.at[1], dev)

    def arrived(dst, sem):
        remote(dst, dst, o_send.at[0], sem, partner).wait_recv()

    def arrived_pair(o_dst, l_dst, sem):
        arrived(o_dst, sem.at[0])
        arrived(l_dst, sem.at[1])

    def send_unit(u):
        r, c, half = ORDER[u]
        o, l = ob.at[u], ol.at[u]
        if r == 2:
            dev = (xl if half == 0 else xr) * CORES + c
            send_pair(o, l, ri.at[half, k], rl.at[half, k], r_recv.at[half, k], dev)
        elif r == 0:
            if c == 'o':
                send_pair(o, l, fp.at[half], fpl.at[half], p_recv.at[half], partner)
        elif (r == -1) == (half == 0):
            if c == 'o':
                send_pair(o, l, ri.at[half, 2], rl.at[half, 2], r_recv.at[half, 2], partner)
        else:
            dev = (xl if r == -1 else xr) * CORES + c
            send_pair(o, l, fb.at[half, k], fbl.at[half, k], b_recv.at[half, k], dev)

    def relay(way):
        for i in range(3):
            arrived_pair(ri.at[way, i], rl.at[way, i], r_recv.at[way, i])
        mine = ORDER.index((-1, 's', 0) if way == 0 else (1, 's', 1))
        ws, rfl[way] = weigh([ol[mine]] + [rl[way, i] for i in range(3)])
        outs = [ob.at[mine]] + [ri.at[way, i] for i in range(3)]
        dev = left if way == 0 else right

        def store(b, acc):
            rf[way, b] = acc

        for p in range(PIECES):
            rows = pl.ds(p * piece, piece)
            merge(outs, ws, p * piece, piece, store)
            send(rf.at[way, rows], ff.at[way, rows], f_recv.at[way, p], dev)
            if p == 0:
                send(rfl.at[way], fl.at[way], f_recv.at[way, PIECES], dev)

    for t in range(units + 2):
        for event in before.get(t, []):
            event()
        stage(t)
        if t >= 2:
            u = t - 2
            start = functools.partial(send_unit, u)
            if t < HOLD_UNTIL:
                held.append(start)
            else:
                start()
        if t == RELAY_AFTER:
            relay(0)
            relay(1)

    for half in range(2):
        arrived_pair(fp.at[half], fpl.at[half], p_recv.at[half])
        for i in range(CORES):
            arrived_pair(fb.at[half, i], fbl.at[half, i], b_recv.at[half, i])
        mine = ORDER.index((0, 's', half))
        ws, lol[half] = weigh([ol[mine], fpl[half]] + [fbl[half, i] for i in range(CORES)])
        outs = [ob.at[mine], fp.at[half]] + [fb.at[half, i] for i in range(CORES)]

        def store_local(b, acc):
            lo[half, b] = acc

        merge(outs, ws, 0, unit, store_local)

    for half in range(2):
        arrived(fl.at[half], f_recv.at[half, PIECES])
    done = []
    both = [weigh([lol[half], fl[half]])[0] for half in range(2)]
    for p in range(PIECES):
        for half in range(2):
            arrived(ff.at[half, pl.ds(p * piece, piece)], f_recv.at[half, p])

            def store(b, acc):
                res[half * unit + b] = acc.astype(BF16)

            merge([lo.at[half], ff.at[half]], both[half], p * piece, piece, store)
            rows = pl.ds(half * unit + p * piece, piece)
            c = pltpu.make_async_copy(res.at[rows], out_hbm.at[rows], o_out.at[half, p])
            c.start()
            done.append(c)

    for c in sends:
        c.wait_send()
    for c in done:
        c.wait()


def solution(mesh):
    group = mesh.shape['dcp']
    chips = group // CORES

    def local_step(q_blk, cache_blk, len_blk):
        batch, per_core, width = q_blk.shape
        page = cache_blk.shape[3]
        latent = width - ROPE_DIM
        heads = per_core * group
        rows = batch // group
        unit = rows // 2
        units = batch // unit
        q_own = jnp.transpose(q_blk, (1, 2, 0))
        cache_own = jnp.transpose(cache_blk[:, 0, 0], (0, 2, 1))
        any_spec = pl.BlockSpec(memory_space=pl.ANY)
        dma = pltpu.SemaphoreType.DMA
        vmem = pltpu.VMEM
        return pl.pallas_call(
            functools.partial(kernel, group),
            out_shape=jax.ShapeDtypeStruct((rows, heads, latent), BF16),
            in_specs=[any_spec] * 3,
            out_specs=any_spec,
            scratch_shapes=[
                vmem((per_core, width, batch), BF16),
                vmem((group, batch // chips, per_core * width), BF16),
                vmem((group, batch // chips, per_core * width), BF16),
                vmem((group, batch // chips, per_core * width), BF16),
                vmem((group, batch // chips, per_core * width), BF16),
                vmem((batch, width, page), BF16),
                vmem((pl.cdiv(width, LANES), heads * unit, LANES), F32),
                vmem((2, unit, heads, page), F32),
                vmem((2, unit, heads, page), BF16),
                vmem((2, unit, heads, page), F32),
                vmem((units, unit, heads, latent), BF16),
                vmem((units, heads // 2, LANES), F32),
                vmem((2, 3, unit, heads, latent), BF16),
                vmem((2, 3, heads // 2, LANES), F32),
                vmem((2, unit, heads, latent), F32),
                vmem((2, heads // 2, LANES), F32),
                vmem((2, unit, heads, latent), F32),
                vmem((2, heads // 2, LANES), F32),
                vmem((2, CORES, unit, heads, latent), BF16),
                vmem((2, CORES, heads // 2, LANES), F32),
                vmem((2, unit, heads, latent), BF16),
                vmem((2, heads // 2, LANES), F32),
                vmem((2, unit, heads, latent), F32),
                vmem((2, heads // 2, LANES), F32),
                pltpu.SMEM((batch,), jnp.int32),
                vmem((rows, heads, latent), BF16),
                dma(()),
                dma(()),
                dma((units,)),
                dma((32,)),
                dma((group, chips)),
                dma((CORES, 2)),
                dma((32,)),
                dma((2, 3, 2)),
                dma((2, PIECES + 1)),
                dma((2, CORES, 2)),
                dma((2, 2)),
                dma((2, PIECES)),
            ],
            compiler_params=pltpu.CompilerParams(collective_id=0, has_side_effects=True,
                                                 vmem_limit_bytes=67043328),
        )(q_own, cache_own, len_blk)

    return jax.shard_map(local_step, mesh=mesh, in_specs=(P('dp', 'dcp', None), P('dp', None, 'dcp', None, None), P('dp')), out_specs=P(('dp', 'dcp'), None, None), check_vma=False)
```

```python
import functools

import jax
import jax.numpy as jnp
from jax import lax
from jax.experimental import pallas as pl
from jax.experimental.pallas import tpu as pltpu
from jax.sharding import PartitionSpec as P

ROPE_DIM = 64
QK_DIM = 192
CORES = 2
LANES = 128
STEP = 8
MERGE_STEP = 4
PIECES = 2
MESH = pl.DeviceIdType.MESH
F32, BF16 = jnp.float32, jnp.bfloat16

ORDER = [(2, 0, 0), (2, 0, 1), (2, 1, 0), (2, 1, 1),
         (1, 'o', 1), (1, 0, 0), (1, 1, 0), (1, 's', 1),
         (-1, 'o', 0), (-1, 0, 1), (-1, 1, 1), (-1, 's', 0),
         (0, 'o', 0), (0, 'o', 1), (0, 's', 0), (0, 's', 1)]
RELAY_AFTER = 15
HOLD_UNTIL = 4
TAIL = 16


def kernel(group, q_ref, cache_ref, len_hbm, res,
           qraw, qb0, qb1, qb2, qb3, cv, q32, sb, wb, ib, ob, ol, ri, rl, rf, rfl, ff, fl, fb, fbl, fp, fpl, lo, lol, len_ref,
           l_in, q_in, c_in, q_send, q_recv, q_tail, o_send, r_recv, f_recv, b_recv, p_recv):
    chips = group // CORES
    batch, width, page = cv.shape
    latent = width - ROPE_DIM
    heads = 2 * group
    blk = batch // chips
    core_rows = batch // group
    unit = core_rows // 2
    units = batch // unit
    piece = unit // PIECES
    scale = QK_DIM ** -0.5

    me = lax.axis_index('dcp')
    x, k = me // CORES, me % CORES
    xr, xl = (x + 1) % chips, (x + chips - 1) % chips
    other = 1 - k
    right, left, partner = xr * CORES + k, xl * CORES + k, x * CORES + other

    def remote(src, dst, send, recv, dev):
        return pltpu.make_async_remote_copy(src_ref=src, dst_ref=dst, send_sem=send, recv_sem=recv,
                                            device_id={'dcp': dev}, device_id_type=MESH)

    def core_of(c):
        return other if c == 'o' else k if c == 's' else c

    def first_row(u):
        r, c, half = ORDER[u]
        return pl.multiple_of((((x + r + chips) % chips) * CORES + core_of(c)) * core_rows + half * unit, unit)

    def cache_copy(u):
        rows = pl.ds(first_row(u), unit)
        return pltpu.make_async_copy(cache_ref.at[rows], cv.at[rows], c_in.at[u])

    blocks = [qb0, qb1, qb2, qb3]
    own_q = pltpu.make_async_copy(q_ref, qraw, q_in)
    own_q.start()
    own_len = pltpu.make_async_copy(len_hbm, len_ref, l_in)
    own_len.start()

    barrier = pltpu.get_barrier_semaphore()
    peers = [partner] + [c * CORES + i for c in (xl, xr) for i in range(CORES)]
    for dev in peers:
        pl.semaphore_signal(barrier, inc=1, device_id={'dcp': dev}, device_id_type=MESH)

    own_q.wait()
    for s in range(chips):
        first = ((x + s) % chips) * blk
        cols = pl.ds(pl.multiple_of(first // LANES * LANES, LANES), LANES)
        pick = jnp.where(lax.broadcasted_iota(jnp.int32, (blk, LANES), 1) == lax.broadcasted_iota(jnp.int32, (blk, LANES), 0) + first % LANES, 1.0, 0.0).astype(BF16)
        parts = [qraw[h, c * LANES:(c + 1) * LANES, cols] for h in range(2) for c in range(latent // LANES)]
        parts.append(jnp.concatenate([qraw[h, latent:, cols] for h in range(2)], axis=0))
        for c, part in enumerate(parts):
            rows = lax.dot_general(pick, part, (((1,), (1,)), ((), ())), preferred_element_type=F32)
            blocks[s][0, :, c * LANES:(c + 1) * LANES] = rows.astype(BF16)
    pl.semaphore_wait(barrier, len(peers))

    sends = []
    ME, RIGHT, FAR, LEFT = 0, 1, 2, 3

    lead = blk - TAIL

    def q_copy(y, col, s, dev, to, to_col, n, sem=None, rows=slice(None)):
        dst = (y - to) % chips * CORES + to_col
        if isinstance(rows, slice):
            rows = pl.ds(0, lead if y - to in (FAR, -FAR) and s in (1, 2) else blk)
        return remote(blocks[(y + s) % chips].at[y * CORES + col, rows], blocks[(y + s - to) % chips].at[dst, rows],
                      q_send.at[n], q_recv.at[dst, s] if sem is None else sem, dev)

    def q_begin(c):
        c.start()
        sends.append(c)

    def q_start(y, s, to):
        dev = {ME: partner, RIGHT: right, LEFT: left}[to]
        q_begin(q_copy(y, 0, s, dev, to, 1 if to == ME else 0, len(sends)))

    def q_wait(y, col, s):
        q_copy(y, col, s, partner, 0, col, 0).wait_recv()

    def go(s, to):
        q_start(ME, s, to)

    def take(y, s, then=None, tail=None):
        q_wait(y, 0, s)
        if then is not None:
            q_start(y, s, then)
        if tail is not None:
            chip = {RIGHT: xr, LEFT: xl}[then]
            for col, core in ((0, k), (1, other)):
                q_begin(q_copy(y, 0, s, chip * CORES + core, then, col, len(sends), q_tail.at[col, tail], pl.ds(lead, TAIL)))
        q_start(y, s, ME)

    def tails():
        for tail, s in ((0, 1), (1, 2)):
            for col in range(CORES):
                q_copy(FAR, col, s, partner, 0, col, 0, q_tail.at[col, tail], pl.ds(lead, TAIL)).wait_recv()

    def from_partner(own, from_left, from_right, from_far):
        for y, s in ((ME, own), (LEFT, from_left), (RIGHT, from_right), (FAR, from_far)):
            q_wait(y, 1, s)

    go(0, RIGHT)
    go(1, LEFT)
    go(3, RIGHT)
    go(3, LEFT)
    go(2, ME)
    go(2, LEFT)
    for u in range(units):
        cache_copy(u).start()
    for s in (1, 3, 0):
        go(s, ME)
    take(LEFT, 0, RIGHT)
    go(1, RIGHT)
    take(RIGHT, 1)
    take(LEFT, 3)
    go(2, RIGHT)
    take(RIGHT, 3, LEFT)
    go(0, LEFT)
    take(FAR, 0)
    take(RIGHT, 2, LEFT, 1)
    from_partner(2, 3, 1, 0)

    own_len.wait()
    held = []

    def slot4():
        take(LEFT, 1, RIGHT, 0)
        take(FAR, 3)

    def slot5():
        take(LEFT, 2)
        take(RIGHT, 0)

    def next_block():
        from_partner(1, 2, 0, 3)

    def slot6():
        take(FAR, 1)
        take(FAR, 2)
        for start in held:
            start()

    def last_blocks():
        tails()
        from_partner(3, 0, 2, 1)
        from_partner(0, 1, 3, 2)

    before = {2: [slot4], 3: [slot5], 4: [slot6, next_block], 8: [last_blocks]}

    lane = lax.broadcasted_iota(jnp.int32, (heads, page), 1)
    position = lane + me * page
    lse_rows = heads // 2
    lse_lane = lax.broadcasted_iota(jnp.int32, (lse_rows, LANES), 1)
    rope_lane = lax.broadcasted_iota(jnp.int32, (unit, LANES), 1)
    of_head = [rope_lane < ROPE_DIM, rope_lane >= ROPE_DIM]

    def stage(t):
        u_qk, u_sm, u_pv = t if t < units else None, t - 1 if 1 <= t <= units else None, t - 2 if t >= 2 else None
        if u_qk is not None:
            row0 = first_row(u_qk)
            cache_copy(u_qk).wait()
            r, c, half = ORDER[u_qk]
            q_block = blocks[r % chips]
            q_rows = pl.ds(pl.multiple_of(core_of(c) * core_rows + half * unit, unit), unit)

            def fill(e, carry):
                d = (x + e // CORES) % chips * CORES + (k + e) % CORES
                for h in range(2):
                    rows = pl.ds(pl.multiple_of((d * 2 + h) * unit, unit), unit)
                    for c in range(latent // LANES):
                        q32[c, rows, :] = q_block[e, q_rows, pl.ds(h * latent + c * LANES, LANES)].astype(F32)
                    rope = q_block[e, q_rows, pl.ds(2 * latent, LANES)].astype(F32)
                    q32[latent // LANES, rows, :] = jnp.where(of_head[h], rope, 0.0)
                return carry

            lax.fori_loop(0, group, fill, 0)
        if u_sm is not None:
            sm_row0 = first_row(u_sm)
        if u_pv is not None:
            pv_row0 = first_row(u_pv)

        def body(i, lse):
            for j in range(STEP):
                b = i * STEP + j
                if u_sm is not None:
                    s = sb[u_sm % 2, b] * scale
                    s = jnp.where(position < len_ref[sm_row0 + b], s, -1e30)
                    m = jnp.max(s, axis=1, keepdims=True)
                    w = jnp.exp(s - m)
                    l = jnp.sum(w, axis=1, keepdims=True)
                    lse_b = m + jnp.log(l)
                    lse = jnp.where(lse_lane == b, lse_b[:lse_rows], jnp.where(lse_lane == b + unit, lse_b[lse_rows:], lse))
                if u_qk is not None:
                    q_b = jnp.concatenate([q32[c, pl.ds(b, heads, stride=unit), :].astype(BF16)
                                           for c in range(latent // LANES + 1)], axis=1)
                    c_b = jnp.concatenate([cv[row0 + b], cv[row0 + b, latent:, :]], axis=0)
                    sb[u_qk % 2, b] = jnp.dot(q_b, c_b, preferred_element_type=F32)
                if u_pv is not None:
                    o = lax.dot_general(wb[u_pv % 2, b], cv[pv_row0 + b, :latent, :], (((1,), (1,)), ((), ())),
                                        preferred_element_type=F32)
                    ob[u_pv, b] = (o * jnp.concatenate([ib[u_pv % 2, b]] * (latent // page), axis=1)).astype(BF16)
                if u_sm is not None:
                    wb[u_sm % 2, b] = w.astype(BF16)
                    ib[u_sm % 2, b] = jnp.broadcast_to(1.0 / l, (heads, page))
            return lse

        lse = lax.fori_loop(0, unit // STEP, body, jnp.zeros((lse_rows, LANES), F32))
        if u_sm is not None:
            ol[u_sm] = lse

    def weigh(ls):
        m = functools.reduce(jnp.maximum, ls)
        es = [jnp.exp(l - m) for l in ls]
        total = functools.reduce(jnp.add, es)
        return [e * (1.0 / total) for e in es], m + jnp.log(total)

    def merge(outs, ws, first, count, store):
        def body(n, carry):
            for j in range(MERGE_STEP):
                b = first + n * MERGE_STEP + j
                acc = None
                for o, w in zip(outs, ws):
                    w_b = jnp.concatenate([jnp.sum(jnp.where(lse_lane == b + i * unit, w, 0.0), axis=1, keepdims=True)
                                           for i in range(2)], axis=0)
                    t = w_b * o[b].astype(F32)
                    acc = t if acc is None else acc + t
                store(b, acc)
            return carry

        lax.fori_loop(0, count // MERGE_STEP, body, 0)

    n_out = [0]

    def send(src, dst, sem, dev):
        c = remote(src, dst, o_send.at[n_out[0]], sem, dev)
        c.start()
        n_out[0] += 1
        sends.append(c)

    def send_pair(o, l, o_dst, l_dst, sem, dev):
        send(o, o_dst, sem.at[0], dev)
        send(l, l_dst, sem.at[1], dev)

    def arrived(dst, sem):
        remote(dst, dst, o_send.at[0], sem, partner).wait_recv()

    def arrived_pair(o_dst, l_dst, sem):
        arrived(o_dst, sem.at[0])
        arrived(l_dst, sem.at[1])

    def send_unit(u):
        r, c, half = ORDER[u]
        o, l = ob.at[u], ol.at[u]
        if r == 2:
            dev = (xl if half == 0 else xr) * CORES + c
            send_pair(o, l, ri.at[half, k], rl.at[half, k], r_recv.at[half, k], dev)
        elif r == 0:
            if c == 'o':
                send_pair(o, l, fp.at[half], fpl.at[half], p_recv.at[half], partner)
        elif (r == -1) == (half == 0):
            if c == 'o':
                send_pair(o, l, ri.at[half, 2], rl.at[half, 2], r_recv.at[half, 2], partner)
        else:
            dev = (xl if r == -1 else xr) * CORES + c
            send_pair(o, l, fb.at[half, k], fbl.at[half, k], b_recv.at[half, k], dev)

    def relay(way):
        for i in range(3):
            arrived_pair(ri.at[way, i], rl.at[way, i], r_recv.at[way, i])
        mine = ORDER.index((-1, 's', 0) if way == 0 else (1, 's', 1))
        ws, rfl[way] = weigh([ol[mine]] + [rl[way, i] for i in range(3)])
        outs = [ob.at[mine]] + [ri.at[way, i] for i in range(3)]
        dev = left if way == 0 else right

        def store(b, acc):
            rf[way, b] = acc

        for p in range(PIECES):
            rows = pl.ds(p * piece, piece)
            merge(outs, ws, p * piece, piece, store)
            send(rf.at[way, rows], ff.at[way, rows], f_recv.at[way, p], dev)
            if p == 0:
                send(rfl.at[way], fl.at[way], f_recv.at[way, PIECES], dev)

    for t in range(units + 2):
        for event in before.get(t, []):
            event()
        stage(t)
        if t >= 2:
            u = t - 2
            start = functools.partial(send_unit, u)
            if t < HOLD_UNTIL:
                held.append(start)
            else:
                start()
        if t == RELAY_AFTER:
            relay(0)
            relay(1)

    for half in range(2):
        arrived_pair(fp.at[half], fpl.at[half], p_recv.at[half])
        for i in range(CORES):
            arrived_pair(fb.at[half, i], fbl.at[half, i], b_recv.at[half, i])
        mine = ORDER.index((0, 's', half))
        ws, lol[half] = weigh([ol[mine], fpl[half]] + [fbl[half, i] for i in range(CORES)])
        outs = [ob.at[mine], fp.at[half]] + [fb.at[half, i] for i in range(CORES)]

        def store_local(b, acc):
            lo[half, b] = acc

        merge(outs, ws, 0, unit, store_local)

    for half in range(2):
        arrived(fl.at[half], f_recv.at[half, PIECES])
    both = [weigh([lol[half], fl[half]])[0] for half in range(2)]
    for p in range(PIECES):
        for half in range(2):
            arrived(ff.at[half, pl.ds(p * piece, piece)], f_recv.at[half, p])

            def store(b, acc):
                res[half * unit + b] = acc.astype(BF16)

            merge([lo.at[half], ff.at[half]], both[half], p * piece, piece, store)
    for c in sends:
        c.wait_send()


def solution(mesh):
    group = mesh.shape['dcp']
    chips = group // CORES

    def local_step(q_blk, cache_blk, len_blk):
        batch, per_core, width = q_blk.shape
        page = cache_blk.shape[3]
        latent = width - ROPE_DIM
        heads = per_core * group
        rows = batch // group
        unit = rows // 2
        units = batch // unit
        q_own = jnp.transpose(q_blk, (1, 2, 0))
        cache_own = jnp.transpose(cache_blk[:, 0, 0], (0, 2, 1))
        any_spec = pl.BlockSpec(memory_space=pl.ANY)
        dma = pltpu.SemaphoreType.DMA
        vmem = pltpu.VMEM
        return pl.pallas_call(
            functools.partial(kernel, group),
            out_shape=pltpu.VMEM((rows, heads, latent), BF16),
            in_specs=[any_spec] * 3,
            out_specs=pl.BlockSpec(memory_space=pltpu.VMEM),
            scratch_shapes=[
                vmem((per_core, width, batch), BF16),
                vmem((group, batch // chips, per_core * width), BF16),
                vmem((group, batch // chips, per_core * width), BF16),
                vmem((group, batch // chips, per_core * width), BF16),
                vmem((group, batch // chips, per_core * width), BF16),
                vmem((batch, width, page), BF16),
                vmem((pl.cdiv(width, LANES), heads * unit, LANES), F32),
                vmem((2, unit, heads, page), F32),
                vmem((2, unit, heads, page), BF16),
                vmem((2, unit, heads, page), F32),
                vmem((units, unit, heads, latent), BF16),
                vmem((units, heads // 2, LANES), F32),
                vmem((2, 3, unit, heads, latent), BF16),
                vmem((2, 3, heads // 2, LANES), F32),
                vmem((2, unit, heads, latent), F32),
                vmem((2, heads // 2, LANES), F32),
                vmem((2, unit, heads, latent), F32),
                vmem((2, heads // 2, LANES), F32),
                vmem((2, CORES, unit, heads, latent), BF16),
                vmem((2, CORES, heads // 2, LANES), F32),
                vmem((2, unit, heads, latent), BF16),
                vmem((2, heads // 2, LANES), F32),
                vmem((2, unit, heads, latent), F32),
                vmem((2, heads // 2, LANES), F32),
                pltpu.SMEM((batch,), jnp.int32),
                dma(()),
                dma(()),
                dma((units,)),
                dma((32,)),
                dma((group, chips)),
                dma((CORES, 2)),
                dma((32,)),
                dma((2, 3, 2)),
                dma((2, PIECES + 1)),
                dma((2, CORES, 2)),
                dma((2, 2)),
            ],
            compiler_params=pltpu.CompilerParams(collective_id=0, has_side_effects=True,
                                                 vmem_limit_bytes=60000000),
        )(q_own, cache_own, len_blk)

    return jax.shard_map(local_step, mesh=mesh, in_specs=(P('dp', 'dcp', None), P('dp', None, 'dcp', None, None), P('dp')), out_specs=P(('dp', 'dcp'), None, None), check_vma=False)
```

```python
import functools

import jax
import jax.numpy as jnp
from jax import lax
from jax.experimental import pallas as pl
from jax.experimental.pallas import tpu as pltpu
from jax.sharding import PartitionSpec as P

ROPE_DIM = 64
QK_DIM = 192
CORES = 2
LANES = 128
STEP = 8
MERGE_STEP = 4
PIECES = 4
MESH = pl.DeviceIdType.MESH
F32, BF16 = jnp.float32, jnp.bfloat16

ORDER = [(2, 0, 0), (2, 0, 1), (2, 1, 0), (2, 1, 1),
         (1, 'o', 1), (1, 0, 0), (1, 1, 0), (1, 's', 1),
         (-1, 'o', 0), (-1, 0, 1), (-1, 1, 1), (-1, 's', 0),
         (0, 'o', 0), (0, 'o', 1), (0, 's', 0), (0, 's', 1)]
RELAY_AFTER = 15
HOLD_UNTIL = 4
TAIL = 16


def kernel(group, q_ref, cache_ref, len_hbm, res,
           qraw, qb0, qb1, qb2, qb3, cv, q32, sb, wb, ib, ob, ol, ri, rl, rf, rfl, ff, fl, fb, fbl, fp, fpl, lo, lol, len_ref,
           l_in, q_in, c_in, q_send, q_recv, q_tail, o_send, r_recv, f_recv, b_recv, p_recv):
    chips = group // CORES
    batch, width, page = cv.shape
    latent = width - ROPE_DIM
    heads = 2 * group
    blk = batch // chips
    core_rows = batch // group
    unit = core_rows // 2
    units = batch // unit
    piece = unit // PIECES
    scale = QK_DIM ** -0.5

    me = lax.axis_index('dcp')
    x, k = me // CORES, me % CORES
    xr, xl = (x + 1) % chips, (x + chips - 1) % chips
    other = 1 - k
    right, left, partner = xr * CORES + k, xl * CORES + k, x * CORES + other

    def remote(src, dst, send, recv, dev):
        return pltpu.make_async_remote_copy(src_ref=src, dst_ref=dst, send_sem=send, recv_sem=recv,
                                            device_id={'dcp': dev}, device_id_type=MESH)

    def core_of(c):
        return other if c == 'o' else k if c == 's' else c

    def first_row(u):
        r, c, half = ORDER[u]
        return pl.multiple_of((((x + r + chips) % chips) * CORES + core_of(c)) * core_rows + half * unit, unit)

    def cache_copy(u):
        rows = pl.ds(first_row(u), unit)
        return pltpu.make_async_copy(cache_ref.at[rows], cv.at[rows], c_in.at[u])

    blocks = [qb0, qb1, qb2, qb3]
    own_q = pltpu.make_async_copy(q_ref, qraw, q_in)
    own_q.start()
    own_len = pltpu.make_async_copy(len_hbm, len_ref, l_in)
    own_len.start()

    barrier = pltpu.get_barrier_semaphore()
    peers = [partner] + [c * CORES + i for c in (xl, xr) for i in range(CORES)]
    for dev in peers:
        pl.semaphore_signal(barrier, inc=1, device_id={'dcp': dev}, device_id_type=MESH)

    own_q.wait()
    for s in range(chips):
        first = ((x + s) % chips) * blk
        cols = pl.ds(pl.multiple_of(first // LANES * LANES, LANES), LANES)
        pick = jnp.where(lax.broadcasted_iota(jnp.int32, (blk, LANES), 1) == lax.broadcasted_iota(jnp.int32, (blk, LANES), 0) + first % LANES, 1.0, 0.0).astype(BF16)
        parts = [qraw[h, c * LANES:(c + 1) * LANES, cols] for h in range(2) for c in range(latent // LANES)]
        parts.append(jnp.concatenate([qraw[h, latent:, cols] for h in range(2)], axis=0))
        for c, part in enumerate(parts):
            rows = lax.dot_general(pick, part, (((1,), (1,)), ((), ())), preferred_element_type=F32)
            blocks[s][0, :, c * LANES:(c + 1) * LANES] = rows.astype(BF16)
    pl.semaphore_wait(barrier, len(peers))

    sends = []
    ME, RIGHT, FAR, LEFT = 0, 1, 2, 3

    lead = blk - TAIL

    def q_copy(y, col, s, dev, to, to_col, n, sem=None, rows=slice(None)):
        dst = (y - to) % chips * CORES + to_col
        if isinstance(rows, slice):
            rows = pl.ds(0, lead if y - to in (FAR, -FAR) and s in (1, 2) else blk)
        return remote(blocks[(y + s) % chips].at[y * CORES + col, rows], blocks[(y + s - to) % chips].at[dst, rows],
                      q_send.at[n], q_recv.at[dst, s] if sem is None else sem, dev)

    def q_begin(c):
        c.start()
        sends.append(c)

    def q_start(y, s, to):
        dev = {ME: partner, RIGHT: right, LEFT: left}[to]
        q_begin(q_copy(y, 0, s, dev, to, 1 if to == ME else 0, len(sends)))

    def q_wait(y, col, s):
        q_copy(y, col, s, partner, 0, col, 0).wait_recv()

    def go(s, to):
        q_start(ME, s, to)

    def take(y, s, then=None, tail=None):
        q_wait(y, 0, s)
        if then is not None:
            q_start(y, s, then)
        if tail is not None:
            chip = {RIGHT: xr, LEFT: xl}[then]
            for col, core in ((0, k), (1, other)):
                q_begin(q_copy(y, 0, s, chip * CORES + core, then, col, len(sends), q_tail.at[col, tail], pl.ds(lead, TAIL)))
        q_start(y, s, ME)

    def tails():
        for tail, s in ((0, 1), (1, 2)):
            for col in range(CORES):
                q_copy(FAR, col, s, partner, 0, col, 0, q_tail.at[col, tail], pl.ds(lead, TAIL)).wait_recv()

    def from_partner(own, from_left, from_right, from_far):
        for y, s in ((ME, own), (LEFT, from_left), (RIGHT, from_right), (FAR, from_far)):
            q_wait(y, 1, s)

    go(0, RIGHT)
    go(1, LEFT)
    go(3, RIGHT)
    go(3, LEFT)
    go(2, ME)
    go(2, LEFT)
    for u in range(units):
        cache_copy(u).start()
    for s in (1, 3, 0):
        go(s, ME)
    take(LEFT, 0, RIGHT)
    go(1, RIGHT)
    take(RIGHT, 1)
    take(LEFT, 3)
    go(2, RIGHT)
    take(RIGHT, 3, LEFT)
    go(0, LEFT)
    take(FAR, 0)
    take(RIGHT, 2, LEFT, 1)
    from_partner(2, 3, 1, 0)

    own_len.wait()
    held = []

    def slot4():
        take(LEFT, 1, RIGHT, 0)
        take(FAR, 3)

    def slot5():
        take(LEFT, 2)
        take(RIGHT, 0)

    def next_block():
        from_partner(1, 2, 0, 3)

    def slot6():
        take(FAR, 1)
        take(FAR, 2)
        for start in held:
            start()

    def last_blocks():
        tails()
        from_partner(3, 0, 2, 1)
        from_partner(0, 1, 3, 2)

    before = {2: [slot4], 3: [slot5], 4: [slot6, next_block], 8: [last_blocks]}

    lane = lax.broadcasted_iota(jnp.int32, (heads, page), 1)
    position = lane + me * page
    lse_rows = heads // 2
    lse_lane = lax.broadcasted_iota(jnp.int32, (lse_rows, LANES), 1)
    rope_lane = lax.broadcasted_iota(jnp.int32, (unit, LANES), 1)
    of_head = [rope_lane < ROPE_DIM, rope_lane >= ROPE_DIM]

    def stage(t):
        u_qk, u_sm, u_pv = t if t < units else None, t - 1 if 1 <= t <= units else None, t - 2 if t >= 2 else None
        if u_qk is not None:
            row0 = first_row(u_qk)
            cache_copy(u_qk).wait()
            r, c, half = ORDER[u_qk]
            q_block = blocks[r % chips]
            q_rows = pl.ds(pl.multiple_of(core_of(c) * core_rows + half * unit, unit), unit)

            def fill(e, carry):
                d = (x + e // CORES) % chips * CORES + (k + e) % CORES
                for h in range(2):
                    rows = pl.ds(pl.multiple_of((d * 2 + h) * unit, unit), unit)
                    for c in range(latent // LANES):
                        q32[c, rows, :] = q_block[e, q_rows, pl.ds(h * latent + c * LANES, LANES)].astype(F32)
                    rope = q_block[e, q_rows, pl.ds(2 * latent, LANES)].astype(F32)
                    q32[latent // LANES, rows, :] = jnp.where(of_head[h], rope, 0.0)
                return carry

            lax.fori_loop(0, group, fill, 0)
        if u_sm is not None:
            sm_row0 = first_row(u_sm)
        if u_pv is not None:
            pv_row0 = first_row(u_pv)

        def body(i, lse):
            for j in range(STEP):
                b = i * STEP + j
                if u_sm is not None:
                    s = sb[u_sm % 2, b] * scale
                    s = jnp.where(position < len_ref[sm_row0 + b], s, -1e30)
                    m = jnp.max(s, axis=1, keepdims=True)
                    w = jnp.exp(s - m)
                    l = jnp.sum(w, axis=1, keepdims=True)
                    lse_b = m + jnp.log(l)
                    lse = jnp.where(lse_lane == b, lse_b[:lse_rows], jnp.where(lse_lane == b + unit, lse_b[lse_rows:], lse))
                if u_qk is not None:
                    q_b = jnp.concatenate([q32[c, pl.ds(b, heads, stride=unit), :].astype(BF16)
                                           for c in range(latent // LANES + 1)], axis=1)
                    c_b = jnp.concatenate([cv[row0 + b], cv[row0 + b, latent:, :]], axis=0)
                    sb[u_qk % 2, b] = jnp.dot(q_b, c_b, preferred_element_type=F32)
                if u_pv is not None:
                    o = lax.dot_general(wb[u_pv % 2, b], cv[pv_row0 + b, :latent, :], (((1,), (1,)), ((), ())),
                                        preferred_element_type=F32)
                    ob[u_pv, b] = (o * jnp.concatenate([ib[u_pv % 2, b]] * (latent // page), axis=1)).astype(BF16)
                if u_sm is not None:
                    wb[u_sm % 2, b] = w.astype(BF16)
                    ib[u_sm % 2, b] = jnp.broadcast_to(1.0 / l, (heads, page))
            return lse

        lse = lax.fori_loop(0, unit // STEP, body, jnp.zeros((lse_rows, LANES), F32))
        if u_sm is not None:
            ol[u_sm] = lse

    def weigh(ls):
        m = functools.reduce(jnp.maximum, ls)
        es = [jnp.exp(l - m) for l in ls]
        total = functools.reduce(jnp.add, es)
        return [e * (1.0 / total) for e in es], m + jnp.log(total)

    def merge(outs, ws, first, count, store):
        def body(n, carry):
            for j in range(MERGE_STEP):
                b = first + n * MERGE_STEP + j
                acc = None
                for o, w in zip(outs, ws):
                    w_b = jnp.concatenate([jnp.sum(jnp.where(lse_lane == b + i * unit, w, 0.0), axis=1, keepdims=True)
                                           for i in range(2)], axis=0)
                    t = w_b * o[b].astype(F32)
                    acc = t if acc is None else acc + t
                store(b, acc)
            return carry

        lax.fori_loop(0, count // MERGE_STEP, body, 0)

    n_out = [0]

    def send(src, dst, sem, dev):
        c = remote(src, dst, o_send.at[n_out[0]], sem, dev)
        c.start()
        n_out[0] += 1
        sends.append(c)

    def send_pair(o, l, o_dst, l_dst, sem, dev):
        send(o, o_dst, sem.at[0], dev)
        send(l, l_dst, sem.at[1], dev)

    def arrived(dst, sem):
        remote(dst, dst, o_send.at[0], sem, partner).wait_recv()

    def arrived_pair(o_dst, l_dst, sem):
        arrived(o_dst, sem.at[0])
        arrived(l_dst, sem.at[1])

    def send_unit(u):
        r, c, half = ORDER[u]
        o, l = ob.at[u], ol.at[u]
        if r == 2:
            dev = (xl if half == 0 else xr) * CORES + c
            send_pair(o, l, ri.at[half, k], rl.at[half, k], r_recv.at[half, k], dev)
        elif r == 0:
            if c == 'o':
                send_pair(o, l, fp.at[half], fpl.at[half], p_recv.at[half], partner)
        elif (r == -1) == (half == 0):
            if c == 'o':
                send_pair(o, l, ri.at[half, 2], rl.at[half, 2], r_recv.at[half, 2], partner)
        else:
            dev = (xl if r == -1 else xr) * CORES + c
            send_pair(o, l, fb.at[half, k], fbl.at[half, k], b_recv.at[half, k], dev)

    def relay(way):
        for i in range(3):
            arrived_pair(ri.at[way, i], rl.at[way, i], r_recv.at[way, i])
        mine = ORDER.index((-1, 's', 0) if way == 0 else (1, 's', 1))
        ws, rfl[way] = weigh([ol[mine]] + [rl[way, i] for i in range(3)])
        outs = [ob.at[mine]] + [ri.at[way, i] for i in range(3)]
        dev = left if way == 0 else right

        def store(b, acc):
            rf[way, b] = acc

        for p in range(PIECES):
            rows = pl.ds(p * piece, piece)
            merge(outs, ws, p * piece, piece, store)
            send(rf.at[way, rows], ff.at[way, rows], f_recv.at[way, p], dev)
            if p == 0:
                send(rfl.at[way], fl.at[way], f_recv.at[way, PIECES], dev)

    for t in range(units + 2):
        for event in before.get(t, []):
            event()
        stage(t)
        if t >= 2:
            u = t - 2
            start = functools.partial(send_unit, u)
            if t < HOLD_UNTIL:
                held.append(start)
            else:
                start()
        if t == RELAY_AFTER:
            relay(0)
            relay(1)

    for half in range(2):
        arrived_pair(fp.at[half], fpl.at[half], p_recv.at[half])
        for i in range(CORES):
            arrived_pair(fb.at[half, i], fbl.at[half, i], b_recv.at[half, i])
        mine = ORDER.index((0, 's', half))
        ws, lol[half] = weigh([ol[mine], fpl[half]] + [fbl[half, i] for i in range(CORES)])
        outs = [ob.at[mine], fp.at[half]] + [fb.at[half, i] for i in range(CORES)]

        def store_local(b, acc):
            lo[half, b] = acc

        merge(outs, ws, 0, unit, store_local)

    for half in range(2):
        arrived(fl.at[half], f_recv.at[half, PIECES])
    both = [weigh([lol[half], fl[half]])[0] for half in range(2)]
    for p in range(PIECES):
        for half in range(2):
            arrived(ff.at[half, pl.ds(p * piece, piece)], f_recv.at[half, p])

            def store(b, acc):
                res[half * unit + b] = acc.astype(BF16)

            merge([lo.at[half], ff.at[half]], both[half], p * piece, piece, store)
    for c in sends:
        c.wait_send()


def solution(mesh):
    group = mesh.shape['dcp']
    chips = group // CORES

    def local_step(q_blk, cache_blk, len_blk):
        batch, per_core, width = q_blk.shape
        page = cache_blk.shape[3]
        latent = width - ROPE_DIM
        heads = per_core * group
        rows = batch // group
        unit = rows // 2
        units = batch // unit
        q_own = jnp.transpose(q_blk, (1, 2, 0))
        cache_own = jnp.transpose(cache_blk[:, 0, 0], (0, 2, 1))
        any_spec = pl.BlockSpec(memory_space=pl.ANY)
        dma = pltpu.SemaphoreType.DMA
        vmem = pltpu.VMEM
        return pl.pallas_call(
            functools.partial(kernel, group),
            out_shape=pltpu.VMEM((rows, heads, latent), BF16),
            in_specs=[any_spec] * 3,
            out_specs=pl.BlockSpec(memory_space=pltpu.VMEM),
            scratch_shapes=[
                vmem((per_core, width, batch), BF16),
                vmem((group, batch // chips, per_core * width), BF16),
                vmem((group, batch // chips, per_core * width), BF16),
                vmem((group, batch // chips, per_core * width), BF16),
                vmem((group, batch // chips, per_core * width), BF16),
                vmem((batch, width, page), BF16),
                vmem((pl.cdiv(width, LANES), heads * unit, LANES), F32),
                vmem((2, unit, heads, page), F32),
                vmem((2, unit, heads, page), BF16),
                vmem((2, unit, heads, page), F32),
                vmem((units, unit, heads, latent), BF16),
                vmem((units, heads // 2, LANES), F32),
                vmem((2, 3, unit, heads, latent), BF16),
                vmem((2, 3, heads // 2, LANES), F32),
                vmem((2, unit, heads, latent), F32),
                vmem((2, heads // 2, LANES), F32),
                vmem((2, unit, heads, latent), F32),
                vmem((2, heads // 2, LANES), F32),
                vmem((2, CORES, unit, heads, latent), BF16),
                vmem((2, CORES, heads // 2, LANES), F32),
                vmem((2, unit, heads, latent), BF16),
                vmem((2, heads // 2, LANES), F32),
                vmem((2, unit, heads, latent), F32),
                vmem((2, heads // 2, LANES), F32),
                pltpu.SMEM((batch,), jnp.int32),
                dma(()),
                dma(()),
                dma((units,)),
                dma((32,)),
                dma((group, chips)),
                dma((CORES, 2)),
                dma((36,)),
                dma((2, 3, 2)),
                dma((2, PIECES + 1)),
                dma((2, CORES, 2)),
                dma((2, 2)),
            ],
            compiler_params=pltpu.CompilerParams(collective_id=0, has_side_effects=True,
                                                 vmem_limit_bytes=60000000),
        )(q_own, cache_own, len_blk)

    return jax.shard_map(local_step, mesh=mesh, in_specs=(P('dp', 'dcp', None), P('dp', None, 'dcp', None, None), P('dp')), out_specs=P(('dp', 'dcp'), None, None), check_vma=False)
```
